256 devices in a mesh: heads: 4 (over x_hi, core), ctx: 64 (over x_lo, z, y).
Axes of the slice: x: 4 (x_hi: 2, x_lo: 2; x = x_hi * 2 + x_lo), y: 4, z: 8, core: 2. Of those that a mesh axis runs over, the one named last changes fastest.
Arguments:
- queries: bfloat16 [12288, 2048], P('ctx', 'heads'), may hold values from -6 to 6
- key_states: bfloat16 [12288, 512], P('ctx', 'heads'), may hold values from -6 to 6
- value_states: bfloat16 [12288, 512], P('ctx', 'heads'), may hold values from -6 to 6
- attention_out: bfloat16 [12288, 2048], P('ctx', 'heads'), may hold values from -2 to 2
- out_grad: bfloat16 [12288, 2048], P('ctx', 'heads'), may hold values from -6 to 6
- log_sum_exp: float32 [16, 12288], P('heads', 'ctx'), may hold values from 0 to 16, as said below
- block_counts: int32 [64], replicated, may hold values from 1 to 3, as said below
- w_query: bfloat16 [4096, 2048], P(None, 'heads'), may hold values from -0.09375 to 0.09375
- w_key: bfloat16 [4096, 512], P(None, 'heads'), may hold values from -0.09375 to 0.09375
- w_value: bfloat16 [4096, 512], P(None, 'heads'), may hold values from -0.09375 to 0.09375
Outputs:
- input_grad: bfloat16 [12288, 4096], P('ctx', 'heads')
- key_grad: float32 [12288, 512], P('ctx', 'heads')
- value_grad: float32 [12288, 512], P('ctx', 'heads')
The draws below stay inside these ranges and needn't reach their ends.
Inputs may be any that keep to these rules, and one draw needn't show every extreme that they name: `block_counts`: one entry equals 3. `log_sum_exp`: finite offsets of each row's scores.
All inputs are finite; a program needn't handle non-finite values.
Results may differ from the reference program's by a relative error of at most 0.0063.
Values may be sent and summed in bfloat16 or wider, within the bound.
A program may use at most 128 MiB of HBM per device.

```python
import math
import jax
import jax.numpy as jnp
from jax import lax

D_MODEL = 4096
HEAD_DIM = 128
GROUP = 4
CAP = 192
BLOCK = 64
KV_HEADS = 4
TOKENS_CAP = 12288
N_CTX = 64


def shared_counts(key):
    count_key = jax.random.fold_in(key, 101)
    pick_key = jax.random.fold_in(key, 202)
    counts = jax.random.randint(count_key, (N_CTX,), 1, CAP // BLOCK + 1, dtype=jnp.int32)
    chosen = jax.random.randint(pick_key, (), 0, N_CTX, dtype=jnp.int32)
    return jnp.where(jnp.arange(N_CTX, dtype=jnp.int32) == chosen, CAP // BLOCK, counts).astype(jnp.int32)


def draw_block_counts(key, part):
    return shared_counts(key)


def draw_log_sum_exp(key, part):
    counts = shared_counts(key)
    lengths = counts * BLOCK
    offsets = jnp.cumsum(lengths) - lengths
    row_index = jnp.arange(CAP * N_CTX, dtype=jnp.int32)
    device = row_index // CAP
    within = row_index - device * CAP
    position = offsets[device] + within
    visible_keys = (position + 1).astype(jnp.float32)
    noise_key = jax.random.fold_in(key, 303)
    base = jax.random.uniform(noise_key, (KV_HEADS * GROUP, CAP * N_CTX), jnp.float32, 0.3, 1.2)
    return jnp.log(visible_keys)[None, :] + base


def steps_of(rng, shape, split, least, high):
    level = 1.0
    for dim, blocks in split:
        steps = jax.random.uniform(jax.random.fold_in(jax.random.fold_in(rng, 6), dim), (blocks,), jnp.float32, least / len(split), high / len(split))
        level = level * jnp.repeat(jnp.exp(steps), shape[dim] // blocks).reshape((-1,) + (1,) * (len(shape) - 1 - dim))
    return level


def bell_draw(rng, shape, spread, reach, pieces=(), held_as=jnp.bfloat16):
    entries = jax.random.normal(rng, shape, jnp.float32) * spread
    if len(pieces) > 0:
        entries = steps_of(rng, shape, pieces, -0.22, 0.18) * entries
    return jnp.clip(entries, min=-reach, max=reach).astype(held_as)


def setup_inputs(seed: int = 0) -> dict:
    splits = jax.random.split(jax.random.key(seed), 11)
    queries = bell_draw(splits[0], (TOKENS_CAP, KV_HEADS * GROUP * HEAD_DIM), 1.0, 6.0, ((0, 64), (1, 4)))
    key_states = bell_draw(splits[1], (TOKENS_CAP, KV_HEADS * HEAD_DIM), 1.0, 6.0, ((0, 64), (1, 4)))
    value_states = bell_draw(splits[2], (TOKENS_CAP, KV_HEADS * HEAD_DIM), 1.0, 6.0, ((0, 64), (1, 4)))
    attention_out = bell_draw(splits[3], (TOKENS_CAP, KV_HEADS * GROUP * HEAD_DIM), 0.3, 2.0, ((0, 64), (1, 4)))
    out_grad = bell_draw(splits[4], (TOKENS_CAP, KV_HEADS * GROUP * HEAD_DIM), 1.0, 6.0, ((0, 64), (1, 4)))
    log_sum_exp = draw_log_sum_exp(jax.random.fold_in(splits[10], 71), 0)
    block_counts = draw_block_counts(jax.random.fold_in(splits[10], 71), 0)
    w_query = bell_draw(splits[7], (D_MODEL, KV_HEADS * GROUP * HEAD_DIM), D_MODEL ** -0.5, 0.09375, ((1, 4),))
    w_key = bell_draw(splits[8], (D_MODEL, KV_HEADS * HEAD_DIM), D_MODEL ** -0.5, 0.09375, ((1, 4),))
    w_value = bell_draw(splits[9], (D_MODEL, KV_HEADS * HEAD_DIM), D_MODEL ** -0.5, 0.09375, ((1, 4),))
    return dict(queries=queries, key_states=key_states, value_states=value_states, attention_out=attention_out, out_grad=out_grad, log_sum_exp=log_sum_exp, block_counts=block_counts, w_query=w_query, w_key=w_key, w_value=w_value)


def slot_table(block_counts):
    lengths = (block_counts * BLOCK).astype(jnp.int32)
    offsets = (jnp.cumsum(lengths) - lengths).astype(jnp.int32)
    row_index = jnp.arange(CAP * N_CTX, dtype=jnp.int32)
    device = row_index // CAP
    within = row_index - device * CAP
    position = offsets[device] + within
    live = within < lengths[device]
    return (position, live)

def reference(queries, key_states, value_states, attention_out, out_grad, log_sum_exp, block_counts, w_query, w_key, w_value):
    total_rows = CAP * N_CTX
    score_scale = 1.0 / math.sqrt(HEAD_DIM)
    position, live = slot_table(block_counts)
    query_block = math.gcd(total_rows, 512)
    width = GROUP * HEAD_DIM
    query_parts = []
    key_parts = []
    value_parts = []
    for head_num in range(KV_HEADS):
        query_h = queries[:, head_num * width:(head_num + 1) * width].reshape(total_rows, GROUP, HEAD_DIM)
        grad_h = out_grad[:, head_num * width:(head_num + 1) * width].reshape(total_rows, GROUP, HEAD_DIM)
        output_h = attention_out[:, head_num * width:(head_num + 1) * width].reshape(total_rows, GROUP, HEAD_DIM)
        key_h = key_states[:, head_num * HEAD_DIM:(head_num + 1) * HEAD_DIM].astype(jnp.float32)
        value_h = value_states[:, head_num * HEAD_DIM:(head_num + 1) * HEAD_DIM].astype(jnp.float32)
        norm_h = log_sum_exp[head_num * GROUP:(head_num + 1) * GROUP]
        delta_h = lax.optimization_barrier(jnp.sum(grad_h.astype(jnp.float32) * output_h.astype(jnp.float32), axis=2))

        def step_block(totals, block_num):
            key_acc, value_acc = totals
            begin_row = (block_num * query_block).astype(jnp.int32)
            query_blk = lax.dynamic_slice_in_dim(query_h, begin_row, query_block, 0).astype(jnp.float32)
            grad_blk = lax.dynamic_slice_in_dim(grad_h, begin_row, query_block, 0).astype(jnp.float32)
            norm_blk = lax.dynamic_slice_in_dim(norm_h, begin_row, query_block, 1)
            delta_blk = lax.dynamic_slice_in_dim(delta_h, begin_row, query_block, 0)
            query_pos = lax.dynamic_slice_in_dim(position, begin_row, query_block, 0)
            query_live = lax.dynamic_slice_in_dim(live, begin_row, query_block, 0)
            scores = jnp.einsum('qgd,kd->gqk', query_blk, key_h) * score_scale
            visible = query_live[:, None] & live[None, :] & (position[None, :] <= query_pos[:, None])
            probability = jnp.where(visible[None], jnp.exp(scores - norm_blk[:, :, None]), 0.0)
            prob_grad = jnp.einsum('qgd,kd->gqk', grad_blk, value_h)
            score_grad = probability * (prob_grad - delta_blk.T[:, :, None])
            prob_b = probability.astype(jnp.bfloat16).astype(jnp.float32)
            grad_b = score_grad.astype(jnp.bfloat16).astype(jnp.float32)
            query_terms = score_scale * jnp.einsum('gqk,kd->qgd', grad_b, key_h)
            key_acc = key_acc + score_scale * jnp.einsum('gqk,qgd->kd', grad_b, query_blk)
            value_acc = value_acc + jnp.einsum('gqk,qgd->kd', prob_b, grad_blk)
            return ((key_acc, value_acc), query_terms)
        zero_keys = jnp.zeros((total_rows, HEAD_DIM), jnp.float32)
        (key_acc, value_acc), grad_blocks = lax.scan(step_block, (zero_keys, zero_keys), jnp.arange(total_rows // query_block, dtype=jnp.int32))
        query_parts.append(grad_blocks.reshape(total_rows, width))
        key_parts.append(key_acc)
        value_parts.append(value_acc)
    query_grad = jnp.concatenate(query_parts, axis=1)
    key_grad = jnp.concatenate(key_parts, axis=1)
    value_grad = jnp.concatenate(value_parts, axis=1)
    input_grad = jnp.dot(query_grad.astype(jnp.bfloat16), w_query.T, preferred_element_type=jnp.float32)
    input_grad = input_grad + jnp.dot(key_grad.astype(jnp.bfloat16), w_key.T, preferred_element_type=jnp.float32)
    input_grad = input_grad + jnp.dot(value_grad.astype(jnp.bfloat16), w_value.T, preferred_element_type=jnp.float32)
    return (input_grad.astype(jnp.bfloat16), key_grad, value_grad)
```

```python
import functools
import math

import jax
import jax.numpy as jnp
from jax import lax
from jax.experimental import pallas as pl
from jax.experimental.pallas import tpu as pltpu
from jax.sharding import PartitionSpec as P

UNIT = 64
CAP = 192
HD = 128
GROUP = 4
NX, NZ, NY = 2, 8, 4
CHUNK = 512
KMAX = NX * NZ * CAP + CHUNK
LOG2E = math.log2(math.e)
SCALE = 1.0 / math.sqrt(HD)
MESH = pl.DeviceIdType.MESH
VMEM = pl.BlockSpec(memory_space=pltpu.VMEM)
SMEM = pl.BlockSpec(memory_space=pltpu.SMEM)
F32 = jnp.float32
BF16 = jnp.bfloat16


def place():
    c = lax.axis_index("ctx")
    return c // (NZ * NY), lax.rem(c // NY, NZ), lax.rem(c, NY)


def ctx_id(x, z, y):
    return {"ctx": (x * NZ + z) * NY + y}


def move(src, dst, send, recv, to):
    return pltpu.make_async_remote_copy(
        src_ref=src, dst_ref=dst, send_sem=send, recv_sem=recv, device_id=to, device_id_type=MESH
    )


def greet(peers):
    barrier = pltpu.get_barrier_semaphore()
    for peer in peers:
        pl.semaphore_signal(barrier, inc=1, device_id=peer, device_id_type=MESH)
    pl.semaphore_wait(barrier, len(peers))


def neighbours(x, z, y):
    return [
        ctx_id(x, lax.rem(z + 1, NZ), y),
        ctx_id(x, lax.rem(z + NZ - 1, NZ), y),
        ctx_id(x, z, lax.rem(y + 1, NY)),
        ctx_id(x, z, lax.rem(y + NY - 1, NY)),
        ctx_id(1 - x, z, y),
    ]


DIRS = (1, -1)
CROSS = (0, 1, -1, 2, -2)


def gather_kernel(
    k_ref, v_ref, q_ref, g_ref, st_ref, kv_out, q_out, g_out, st_out,
    zs, zr, es, er, xs, xr, ys, yr,
):
    x, z, y = place()
    greet(neighbours(x, z, y))
    own = (k_ref, v_ref)

    def zz(k):
        return lax.rem(z + k + NZ, NZ)

    def ring(d, p, s):
        slot = x * NZ + zz(-DIRS[d] * s)
        src = own[p] if s == 0 else kv_out.at[slot, p]
        return move(src, kv_out.at[slot, p], zs.at[d, p, s], zr.at[d, p, s], ctx_id(x, zz(DIRS[d]), y))

    def extra(d, p, s):
        slot = zz(-DIRS[d] * s)
        return move(
            kv_out.at[slot, p], kv_out.at[slot, p], es.at[d, p, s - 2], er.at[d, p, s - 2],
            ctx_id(1, zz(DIRS[d]), y),
        )

    def cross(i, p):
        slot = zz(CROSS[i])
        src = own[p] if i == 0 else kv_out.at[slot, p]
        return move(src, kv_out.at[slot, p], xs.at[i, p], xr.at[i, p], ctx_id(1, z, y))

    def received(i, p):
        slot = zz(CROSS[i])
        return move(kv_out.at[slot, p], kv_out.at[slot, p], xs.at[i, p], xr.at[i, p], ctx_id(0, z, y))

    sources = (q_ref, g_ref, st_ref)
    targets = (q_out, g_out, st_out)

    def yy(k):
        return lax.rem(y + k + NY, NY)

    def side(d, a):
        return move(
            sources[a], targets[a].at[y], ys.at[d, a, 0], yr.at[d, a, 0], ctx_id(x, z, yy(DIRS[d]))
        )

    def far(d, a):
        slot = yy(-DIRS[d])
        return move(
            targets[a].at[slot], targets[a].at[slot], ys.at[d, a, 1], yr.at[d, a, 1],
            ctx_id(x, z, yy(DIRS[d])),
        )

    def valid(d, p, s):
        return s < 3 or d == p

    for p in range(2):
        for d in range(2):
            ring(d, p, 0).start()

    @pl.when(x == 0)
    def _():
        for p in range(2):
            cross(0, p).start()

    side(0, 0).start()
    side(1, 1).start()
    side(0, 2).start()
    side(1, 0).start()
    side(0, 1).start()
    side(1, 2).start()
    kv_out[x * NZ + z, 0] = k_ref[...]
    kv_out[x * NZ + z, 1] = v_ref[...]
    q_out[y] = q_ref[...]
    g_out[y] = g_ref[...]
    st_out[y] = st_ref[...]

    for s in range(1, 3):
        for p in range(2):
            for d in range(2):
                ring(d, p, s - 1).wait_recv()
                ring(d, p, s).start() if valid(d, p, s) else None

                @pl.when(x == 0)
                def _():
                    cross(CROSS.index(-DIRS[d] * s), p).start()

    side(0, 0).wait_recv()
    far(0, 0).start()
    side(1, 1).wait_recv()
    far(1, 1).start()
    side(0, 2).wait_recv()
    far(0, 2).start()
    for p in range(2):
        for d in range(2):
            ring(d, p, 2).wait_recv()
            if valid(d, p, 3):
                ring(d, p, 3).start()

    @pl.when(x == 1)
    def _():
        for p in range(2):
            for d in range(2):
                received(CROSS.index(-DIRS[d] * 2), p).wait_recv()
                extra(d, p, 2).start()
        for p in range(2):
            for d in range(2):
                extra(d, p, 2).wait_recv()
                if valid(d, p, 3):
                    extra(d, p, 3).start()
        for p in range(2):
            for i in range(3):
                received(i, p).wait_recv()
        for p in range(2):
            extra(p, p, 3).wait_recv()

    for p in range(2):
        ring(p, p, 3).wait_recv()
    side(1, 0).wait_recv()
    side(0, 1).wait_recv()
    side(1, 2).wait_recv()
    far(0, 0).wait_recv()
    far(1, 1).wait_recv()
    far(0, 2).wait_recv()

    for s in range(4):
        for p in range(2):
            for d in range(2):
                if valid(d, p, s):
                    ring(d, p, s).wait_send()
    for d in range(2):
        for a in range(3):
            side(d, a).wait_send()
    far(0, 0).wait_send()
    far(1, 1).wait_send()
    far(0, 2).wait_send()

    @pl.when(x == 0)
    def _():
        for p in range(2):
            for i in range(5):
                cross(i, p).wait_send()

    @pl.when(x == 1)
    def _():
        for p in range(2):
            for d in range(2):
                extra(d, p, 2).wait_send()
            extra(p, p, 3).wait_send()


def gather(k, v, q, g, st):
    dma = pltpu.SemaphoreType.DMA
    return pl.pallas_call(
        gather_kernel,
        name="gather_blocks",
        out_shape=(
            jax.ShapeDtypeStruct((NX * NZ, 2, CAP, HD), BF16),
            jax.ShapeDtypeStruct((NY, CAP, GROUP * HD), BF16),
            jax.ShapeDtypeStruct((NY, CAP, GROUP * HD), BF16),
            jax.ShapeDtypeStruct((NY, 8, GROUP * UNIT), F32),
        ),
        in_specs=[VMEM] * 5,
        out_specs=(VMEM,) * 4,
        scratch_shapes=[
            dma((2, 2, 4)), dma((2, 2, 4)), dma((2, 2, 2)), dma((2, 2, 2)),
            dma((5, 2)), dma((5, 2)), dma((2, 3, 2)), dma((2, 3, 2)),
        ],
        compiler_params=pltpu.CompilerParams(collective_id=0, has_side_effects=True),
    )(k, v, q, g, st)


def dot(a, b, dims):
    return lax.dot_general(a, b, (dims, ((), ())), preferred_element_type=F32)


def attention_kernel(
    count_ref, kv_ref, q_ref, g_ref, st_ref, dkv_out, dq_out, kc, vc, kt, dk, dv, dqt, starts
):
    x, z, y = place()
    mine = x * NZ + z

    def block_of(j):
        return j * NY + y

    def pack(j, n):
        starts[j] = n
        at = pl.ds(pl.multiple_of(n * UNIT, UNIT), CAP)
        kc[at, :] = kv_ref[j, 0]
        vc[at, :] = kv_ref[j, 1]
        return n + count_ref[block_of(j)]

    total = lax.fori_loop(0, mine + 1, pack, 0)
    tail = pl.ds(pl.multiple_of(total * UNIT, UNIT), CHUNK)
    kc[tail, :] = jnp.zeros((CHUNK, HD), BF16)
    vc[tail, :] = jnp.zeros((CHUNK, HD), BF16)
    chunks = (total * UNIT + CHUNK - 1) // CHUNK

    @pl.loop(0, chunks)
    def _(ci):
        rows = pl.ds(pl.multiple_of(ci * CHUNK, CHUNK), CHUNK)
        kt[ci] = kc[rows, :].T
        dk[rows, :] = jnp.zeros((CHUNK, HD), F32)
        dv[rows, :] = jnp.zeros((CHUNK, HD), F32)

    before = starts[mine]
    lane = lax.rem(lax.broadcasted_iota(jnp.int32, (1, GROUP * UNIT), 1), UNIT)
    heads = [slice(h * HD, (h + 1) * HD) for h in range(GROUP)]

    @pl.loop(0, NY)
    def _(b):
        live = count_ref[mine * NY + b]
        dq_out[b] = jnp.zeros((CAP, GROUP * HD), BF16)

        @pl.loop(0, live)
        def _(u):
            at = pl.ds(pl.multiple_of(u * UNIT, UNIT), UNIT)
            qn = jnp.concatenate([q_ref[b, at, h] for h in heads], axis=0)
            gn = jnp.concatenate([g_ref[b, at, h] for h in heads], axis=0)
            norm = st_ref[b, pl.ds(u, 1), :]
            delta = st_ref[b, pl.ds(u + 4, 1), :]
            here = jnp.where(b > y, count_ref[block_of(mine)], jnp.where(b == y, u + 1, 0))
            seen = before + here
            limit = (seen - 1) * UNIT + jnp.where(b == y, lane, UNIT - 1)
            dqt[...] = jnp.zeros_like(dqt)

            def step(ci, masked):
                for half in range(CHUNK // 256):
                    first = ci * CHUNK + half * 256
                    rows = pl.ds(pl.multiple_of(first, 256), 256)
                    s = dot(kc[rows, :], qn, ((1,), (1,)))
                    prob = jnp.exp2(s * (SCALE * LOG2E) - norm)
                    if masked:
                        key = first + lax.broadcasted_iota(jnp.int32, prob.shape, 0)
                        prob = jnp.where(key <= limit, prob, 0.0)
                    dp = dot(vc[rows, :], gn, ((1,), (1,)))
                    ds = (prob * (dp - delta)).astype(BF16)
                    dv[rows, :] += dot(prob.astype(BF16), gn, ((1,), (0,)))
                    dk[rows, :] += dot(ds, qn, ((1,), (0,)))
                    dqt[...] += dot(kt[ci, :, half * 256:(half + 1) * 256], ds, ((1,), (0,)))

            full = jnp.maximum(seen - 1, 0) * UNIT // CHUNK
            whole = (seen * UNIT + CHUNK - 1) // CHUNK

            @pl.loop(0, full)
            def _(ci):
                step(ci, False)

            @pl.loop(full, whole)
            def _(ci):
                step(ci, True)

            dq = (dqt[...].T * SCALE).astype(BF16)
            for i, h in enumerate(heads):
                dq_out[b, at, h] = dq[i * UNIT:(i + 1) * UNIT]

    @pl.loop(0, NX * NZ)
    def _(j):
        @pl.when(j <= mine)
        def _():
            at = pl.ds(pl.multiple_of(starts[j] * UNIT, UNIT), CAP)
            row = lax.broadcasted_iota(jnp.int32, (CAP, HD), 0)
            keep = row < count_ref[block_of(j)] * UNIT
            dkv_out[j, 0] = jnp.where(keep, dk[at, :] * SCALE, 0.0).astype(BF16)
            dkv_out[j, 1] = jnp.where(keep, dv[at, :], 0.0).astype(BF16)

        @pl.when(j > mine)
        def _():
            dkv_out[j] = jnp.zeros((2, CAP, HD), BF16)


def attention(counts, kv, q, g, st):
    return pl.pallas_call(
        attention_kernel,
        name="attention_grads",
        out_shape=(
            jax.ShapeDtypeStruct((NX * NZ, 2, CAP, HD), BF16),
            jax.ShapeDtypeStruct((NY, CAP, GROUP * HD), BF16),
        ),
        in_specs=[SMEM] + [VMEM] * 4,
        out_specs=(VMEM,) * 2,
        scratch_shapes=[
            pltpu.VMEM((KMAX, HD), BF16),
            pltpu.VMEM((KMAX, HD), BF16),
            pltpu.VMEM((KMAX // CHUNK, HD, CHUNK), BF16),
            pltpu.VMEM((KMAX, HD), F32),
            pltpu.VMEM((KMAX, HD), F32),
            pltpu.VMEM((HD, GROUP * UNIT), F32),
            pltpu.SMEM((NX * NZ,), jnp.int32),
        ],
    )(counts, kv, q, g, st)


def reduce_kernel(
    p_ref, q_ref, dk_out, dv_out, dq_out,
    zst, zrb, est, erb, xst, xrb, yst, yrb, fst,
    zs, zr, es, er, xs, xr, ys, yr, fs, fr,
):
    x, z, y = place()
    greet(neighbours(x, z, y))

    def zz(k):
        return lax.rem(z + k + NZ, NZ)

    def yy(k):
        return lax.rem(y + k + NY, NY)

    def valid(d, p, s):
        return s > 0 or d == p

    def part(row, d, s, p):
        return p_ref.at[row * NZ + zz(DIRS[d] * (4 - s)), p]

    def joins(d, p, s):
        return s > 0 and valid(d, p, s - 1)

    def ring(d, p, s, src=None):
        src = zst.at[d, p, s] if src is None else src
        return move(src, zrb.at[d, p, s], zs.at[d, p, s], zr.at[d, p, s], ctx_id(x, zz(DIRS[d]), y))

    def extra(d, p, s, src=None):
        src = est.at[d, p, s] if src is None else src
        return move(src, erb.at[d, p, s], es.at[d, p, s], er.at[d, p, s], ctx_id(1, zz(DIRS[d]), y))

    def cross(i, p, src=None):
        src = xst.at[i - 3, p] if src is None else src
        return move(src, xrb.at[i, p], xs.at[i, p], xr.at[i, p], ctx_id(0, z, y))

    def crossed(i, p):
        return move(xrb.at[i, p], xrb.at[i, p], xs.at[i, p], xr.at[i, p], ctx_id(1, z, y))

    half = CAP // 2
    rows = (slice(0, half), slice(half, CAP))

    def far(d):
        return move(
            q_ref.at[yy(2), rows[d]], fst.at[d], fs.at[d], fr.at[d], ctx_id(x, z, yy(DIRS[d]))
        )

    def side(d, joined):
        r = d if joined else 1 - d
        src = yst.at[d] if joined else q_ref.at[yy(DIRS[d]), rows[r]]
        return move(
            src, yrb.at[d, rows[r]], ys.at[d, r], yr.at[d, r], ctx_id(x, z, yy(DIRS[d]))
        )

    for d in range(2):
        ring(d, d, 0, part(x, d, 0, d)).start()

        @pl.when(x == 1)
        def _():
            extra(d, d, 0, part(0, d, 0, d)).start()

        ring(d, 1 - d, 1, part(x, d, 1, 1 - d)).start()

        @pl.when(x == 1)
        def _():
            extra(d, 1 - d, 1, part(0, d, 1, 1 - d)).start()

        far(d).start()

    @pl.when(x == 1)
    def _():
        for p in range(2):
            for i in range(3):
                cross(i, p, p_ref.at[zz(CROSS[i]), p]).start()

    for d in range(2):
        side(d, False).start()

    def add(*refs):
        total = refs[0][...].astype(F32)
        for r in refs[1:]:
            total = total + r[...].astype(F32)
        return total

    for d in range(2):
        @pl.when(x == 1)
        def _():
            extra(d, d, 0, part(0, d, 0, d)).wait_recv()
            est[d, d, 1] = add(part(0, d, 1, d), erb.at[d, d, 0]).astype(BF16)
            extra(d, d, 1).start()

        ring(d, d, 0, part(x, d, 0, d)).wait_recv()
        zst[d, d, 1] = add(part(x, d, 1, d), zrb.at[d, d, 0]).astype(BF16)
        ring(d, d, 1).start()

    @pl.when(x == 1)
    def _():
        for p in range(2):
            for d in range(2):
                i = CROSS.index(2 * DIRS[d])
                extra(d, p, 1).wait_recv()
                xst[i - 3, p] = add(part(0, d, 2, p), erb.at[d, p, 1]).astype(BF16)
                cross(i, p).start()

    for d in range(2):
        far(d).wait_recv()
        yst[d] = add(q_ref.at[yy(DIRS[d]), rows[d]], fst.at[d]).astype(BF16)
        side(d, True).start()

    for s in range(2, 4):
        for p in range(2):
            for d in range(2):
                ring(d, p, s - 1).wait_recv()

                @pl.when(x == 0)
                def _():
                    i = CROSS.index((4 - s) * DIRS[d])
                    crossed(i, p).wait_recv()
                    zst[d, p, s] = add(part(x, d, s, p), zrb.at[d, p, s - 1], xrb.at[i, p]).astype(BF16)

                @pl.when(x == 1)
                def _():
                    zst[d, p, s] = add(part(x, d, s, p), zrb.at[d, p, s - 1]).astype(BF16)

                ring(d, p, s).start()

    for d in range(2):
        side(d, False).wait_recv()
        side(d, True).wait_recv()
    dq_out[...] = add(q_ref.at[y], yrb.at[0], yrb.at[1]).astype(BF16)

    outs = (dk_out, dv_out)
    for p in range(2):
        for d in range(2):
            ring(d, p, 3).wait_recv()

        @pl.when(x == 0)
        def _():
            crossed(0, p).wait_recv()
            outs[p][...] = add(p_ref.at[z, p], zrb.at[0, p, 3], zrb.at[1, p, 3], xrb.at[0, p])

        @pl.when(x == 1)
        def _():
            outs[p][...] = add(p_ref.at[NZ + z, p], zrb.at[0, p, 3], zrb.at[1, p, 3])

    for p in range(2):
        for d in range(2):
            for s in range(4):
                if valid(d, p, s):
                    ring(d, p, s).wait_send()

        @pl.when(x == 1)
        def _():
            for d in range(2):
                for s in range(2):
                    if valid(d, p, s):
                        extra(d, p, s).wait_send()
            for i in range(5):
                cross(i, p, xrb.at[i, p]).wait_send()

    for d in range(2):
        far(d).wait_send()
        side(d, False).wait_send()
        side(d, True).wait_send()


def reduce_blocks(parts, q_parts):
    dma = pltpu.SemaphoreType.DMA
    tile = (CAP, HD)
    return pl.pallas_call(
        reduce_kernel,
        name="reduce_blocks",
        out_shape=(
            jax.ShapeDtypeStruct(tile, F32),
            jax.ShapeDtypeStruct(tile, F32),
            jax.ShapeDtypeStruct((CAP, GROUP * HD), BF16),
        ),
        in_specs=[VMEM] * 2,
        out_specs=(VMEM,) * 3,
        scratch_shapes=[
            pltpu.VMEM((2, 2, 4) + tile, BF16),
            pltpu.VMEM((2, 2, 4) + tile, BF16),
            pltpu.VMEM((2, 2, 2) + tile, BF16),
            pltpu.VMEM((2, 2, 2) + tile, BF16),
            pltpu.VMEM((2, 2) + tile, BF16),
            pltpu.VMEM((5, 2) + tile, BF16),
            pltpu.VMEM((2, CAP // 2, GROUP * HD), BF16),
            pltpu.VMEM((2, CAP, GROUP * HD), BF16),
            pltpu.VMEM((2, CAP // 2, GROUP * HD), BF16),
            dma((2, 2, 4)), dma((2, 2, 4)), dma((2, 2, 2)), dma((2, 2, 2)),
            dma((5, 2)), dma((5, 2)), dma((2, 2)), dma((2, 2)), dma((2,)), dma((2,)),
        ],
        compiler_params=pltpu.CompilerParams(collective_id=1, has_side_effects=True),
    )(parts, q_parts)


def heads_kernel(
    p_ref, out_ref, near, farb, stage, relay, last, cs, cr, rs, rr, ls, lr
):
    hd = lax.axis_index("heads")
    x_lo, z, y = place()
    x_hi, core = hd // 2, lax.rem(hd, 2)
    xx = x_hi * 2 + x_lo
    width = out_ref.shape[1]

    def device(k):
        to = lax.rem(xx + k + 4, 4)
        return {"heads": (to // 2) * 2 + core, **ctx_id(lax.rem(to, 2), z, y)}

    partner = {"heads": x_hi * 2 + 1 - core}
    greet([partner, device(1), device(-1)])

    def columns(hi, c):
        return pl.ds(pl.multiple_of((hi * 2 + c) * width, width), width)

    pieces = 4
    height = CAP // pieces
    rows = [pl.ds(i * height, height) for i in range(pieces)]

    def swap(i, which):
        hi = 1 - x_hi if which == 0 else x_hi
        dst = farb if which == 0 else near
        return move(
            p_ref.at[rows[i], columns(hi, 1 - core)], dst.at[rows[i]], cs.at[which, i], cr.at[which, i], partner
        )

    def hop(i):
        d = DIRS[i % 2]
        return move(stage.at[rows[i]], relay.at[rows[i]], rs.at[i], rr.at[i], device(d))

    def forward(i):
        d = DIRS[i % 2]
        return move(relay.at[rows[i]], last.at[rows[i]], ls.at[i], lr.at[i], device(d))

    for which in range(2):
        for i in range(pieces):
            swap(i, which).start()
    for i in range(pieces):
        swap(i, 0).wait_recv()
        own = p_ref[rows[i], columns(1 - x_hi, core)].astype(F32)
        stage[rows[i]] = (own + farb[rows[i]].astype(F32)).astype(BF16)
        hop(i).start()
    for i in range(pieces):
        hop(i).wait_recv()
        forward(i).start()
    for i in range(pieces):
        swap(i, 1).wait_recv()
    for i in range(pieces):
        forward(i).wait_recv()
        own = p_ref[rows[i], columns(x_hi, core)].astype(F32)
        out_ref[rows[i]] = (own + near[rows[i]].astype(F32) + last[rows[i]].astype(F32)).astype(BF16)
    for i in range(pieces):
        swap(i, 0).wait_send()
        swap(i, 1).wait_send()
        hop(i).wait_send()
        forward(i).wait_send()


def sum_heads(partial):
    dma = pltpu.SemaphoreType.DMA
    block = (CAP, partial.shape[1] // 4)
    return pl.pallas_call(
        heads_kernel,
        name="sum_heads",
        out_shape=jax.ShapeDtypeStruct(block, BF16),
        in_specs=[VMEM],
        out_specs=VMEM,
        scratch_shapes=[pltpu.VMEM(block, BF16)] * 5
        + [dma((2, 4)), dma((2, 4)), dma((4,)), dma((4,)), dma((4,)), dma((4,))],
        compiler_params=pltpu.CompilerParams(collective_id=2, has_side_effects=True),
    )(partial)


def on_device(q, k, v, o, g, lse, counts, wq, wk, wv):
    per_unit = CAP // UNIT
    delta = jnp.sum((g.astype(F32) * o.astype(F32)).reshape(CAP, GROUP, HD), axis=2)
    delta = delta.reshape(per_unit, UNIT, GROUP).transpose(0, 2, 1).reshape(per_unit, GROUP * UNIT)
    norm = (lse * LOG2E).reshape(GROUP, per_unit, UNIT).transpose(1, 0, 2)
    norm = norm.reshape(per_unit, GROUP * UNIT)
    gap = jnp.zeros((1, GROUP * UNIT), F32)
    st = jnp.concatenate([norm, gap, delta, gap], axis=0)
    kv_all, q_all, g_all, st_all = gather(k, v, q, g, st)
    parts, q_parts = attention(counts, kv_all, q_all, g_all, st_all)
    dk, dv, dq = reduce_blocks(parts, q_parts)
    mul = functools.partial(jnp.einsum, "rc,mc->rm", preferred_element_type=F32)
    partial = mul(dq, wq) + mul(dk.astype(BF16), wk) + mul(dv.astype(BF16), wv)
    return sum_heads(partial.astype(BF16)), dk, dv


def solution(mesh):
    return jax.shard_map(
        on_device,
        mesh=mesh,
        in_specs=(
            P("ctx", "heads"), P("ctx", "heads"), P("ctx", "heads"), P("ctx", "heads"), P("ctx", "heads"),
            P("heads", "ctx"), P(), P(None, "heads"), P(None, "heads"), P(None, "heads"),
        ),
        out_specs=(P("ctx", "heads"), P("ctx", "heads"), P("ctx", "heads")),
        check_vma=False,
    )
```

```python
import math

import jax
import jax.numpy as jnp
from jax import lax
from jax.experimental import pallas as pl
from jax.experimental.pallas import tpu as pltpu
from jax.sharding import PartitionSpec as P

UNIT = 64
CAP = 192
HD = 128
GROUP = 4
NX, NZ, NY = 2, 8, 4
TILE = 256
PIECES = 6
LOG2E = math.log2(math.e)
SCALE = 1.0 / math.sqrt(HD)
MESH = pl.DeviceIdType.MESH
VMEM = pl.BlockSpec(memory_space=pltpu.VMEM)
SMEM = pl.BlockSpec(memory_space=pltpu.SMEM)
F32 = jnp.float32
BF16 = jnp.bfloat16


def place():
    c = lax.axis_index("ctx")
    return c // (NZ * NY), lax.rem(c // NY, NZ), lax.rem(c, NY)


def ctx_id(x, z, y):
    return {"ctx": (x * NZ + z) * NY + y}


def move(src, dst, send, recv, to):
    return pltpu.make_async_remote_copy(
        src_ref=src, dst_ref=dst, send_sem=send, recv_sem=recv, device_id=to, device_id_type=MESH
    )


def greet(peers):
    barrier = pltpu.get_barrier_semaphore()
    for peer in peers:
        pl.semaphore_signal(barrier, inc=1, device_id=peer, device_id_type=MESH)
    pl.semaphore_wait(barrier, len(peers))


DIRS = (1, -1)
CROSS = (0, 1, -1, 2, -2)


def weight_copies(w_refs, buf, sems, first):
    copies = []
    for c in range(buf.shape[0]):
        rows, at, group = pl.ds(pl.multiple_of(first + c * TILE, TILE), TILE), 0, []
        for i, w in enumerate(w_refs):
            width = w.shape[1]
            group.append(pltpu.make_async_copy(w.at[rows], buf.at[c, :, at:at + width], sems.at[c, i]))
            at += width
        copies.append(group)
    for group in copies:
        for copy in group:
            copy.start()
    return copies


def dot(a, b, dims):
    return lax.dot_general(a, b, (dims, ((), ())), preferred_element_type=F32)


def fused_kernel(
    count_ref, k_ref, v_ref, q_ref, g_ref, o_ref, lse_ref, wq, wk, wv,
    out_ref, dk_out, dv_out,
    kv, qa, ga, st, kt, acc, dqt, pb, db,
    zst, zrb, est, erb, xst, xrb, fst, frb, yst, yrb,
    act, far, near, farb, nearb, stage, relay, last, wbuf,
    gz, gx, gy, sz, sx, sy, hs, wsem,
):
    hd = lax.axis_index("heads")
    x, z, y = place()
    x_hi, core = hd // 2, lax.rem(hd, 2)
    xx = x_hi * 2 + x
    width = out_ref.shape[1]
    tiles = wbuf.shape[0] // 2
    UNITS = CAP // UNIT
    own = (k_ref, v_ref)

    def zz(k):
        return lax.rem(z + k + NZ, NZ)

    def yy(k):
        return lax.rem(y + k + NY, NY)

    def device(k):
        to = lax.rem(xx + k + 4, 4)
        return {"heads": (to // 2) * 2 + core, **ctx_id(lax.rem(to, 2), z, y)}

    partner = {"heads": x_hi * 2 + 1 - core}

    def along_z(d):
        return ctx_id(x, zz(DIRS[d]), y)

    def along_y(d):
        return ctx_id(x, z, yy(DIRS[d]))

    twin = ctx_id(1 - x, z, y)
    greet([along_z(0), along_z(1), along_y(0), along_y(1), partner, device(1), device(-1)])

    def ring(d, p, s):
        slot = x * NZ + zz(-DIRS[d] * s)
        src = own[p] if s == 0 else kv.at[slot, p]
        return move(src, kv.at[slot, p], gz.at[0, 0, d, p, s], gz.at[0, 1, d, p, s], along_z(d))

    def extra(d, p, s):
        slot = zz(-DIRS[d] * s)
        return move(kv.at[slot, p], kv.at[slot, p], gz.at[1, 0, d, p, s], gz.at[1, 1, d, p, s], along_z(d))

    def cross(i, p):
        slot = zz(CROSS[i])
        src = own[p] if i == 0 else kv.at[slot, p]
        return move(src, kv.at[slot, p], gx.at[0, i, p], gx.at[1, i, p], twin)

    def crossed(i, p):
        slot = zz(CROSS[i])
        return move(kv.at[slot, p], kv.at[slot, p], gx.at[0, i, p], gx.at[1, i, p], twin)

    sources, targets = (q_ref, g_ref, st.at[y]), (qa, ga, st)

    def side(d, a):
        return move(sources[a], targets[a].at[y], gy.at[0, 0, d, a], gy.at[0, 1, d, a], along_y(d))

    def far_side(d, a):
        slot = yy(-DIRS[d])
        return move(
            targets[a].at[slot], targets[a].at[slot], gy.at[1, 0, d, a], gy.at[1, 1, d, a], along_y(d)
        )

    def valid(d, p, s):
        return s < 3 or d == p

    for p in range(2):
        for d in range(2):
            ring(d, p, 0).start()

    @pl.when(x == 0)
    def _():
        for p in range(2):
            cross(0, p).start()

    side(0, 0).start()
    side(1, 1).start()
    side(1, 0).start()
    side(0, 1).start()
    kv[x * NZ + z, 0] = k_ref[...]
    kv[x * NZ + z, 1] = v_ref[...]
    qa[y] = q_ref[...]
    ga[y] = g_ref[...]
    st[y] = jnp.zeros(st.shape[1:], F32)
    for h in range(GROUP):
        cols = slice(h * HD, (h + 1) * HD)
        both = g_ref[:, cols].astype(F32) * o_ref[:, cols].astype(F32)
        delta = jnp.sum(both.T, axis=0, keepdims=True)
        norm = lse_ref[h:h + 1, :] * LOG2E
        for u in range(UNITS):
            part = slice(u * UNIT, (u + 1) * UNIT)
            into = slice(h * UNIT, (h + 1) * UNIT)
            st[y, u:u + 1, into] = norm[:, part]
            st[y, u + 4:u + 5, into] = delta[:, part]
    side(0, 2).start()
    side(1, 2).start()
    dqt[...] = jnp.zeros_like(dqt)

    lane = lax.rem(lax.broadcasted_iota(jnp.int32, (1, GROUP * UNIT), 1), UNIT)
    key = lax.broadcasted_iota(jnp.int32, (CAP, GROUP * UNIT), 0)
    heads = [slice(h * HD, (h + 1) * HD) for h in range(GROUP)]

    def block(keys, query_blocks, fresh):
        slots = [row * NZ + zz(e) for row, e in keys]
        units = [(b, u) for b in query_blocks for u in range(UNITS)]
        if fresh:
            for slot in slots:
                kt[slot] = kv[slot, 0].T

        def operands(i):
            b, u = units[i]
            at = slice(u * UNIT, (u + 1) * UNIT)
            qn = jnp.concatenate([qa[b, at, h] for h in heads], axis=0)
            gn = jnp.concatenate([ga[b, at, h] for h in heads], axis=0)
            return qn, gn

        def products(i):
            qn, gn = operands(i)
            return [(dot(kv[s, 0], qn, ((1,), (1,))), dot(kv[s, 1], gn, ((1,), (1,)))) for s in slots]

        def weights(i, out):
            b, u = units[i]
            norm, delta = st[b, u:u + 1, :], st[b, u + 4:u + 5, :]
            query_block = (x * NZ + z) * NY + b
            query_len = count_ref[query_block] * UNIT
            row_in = u * UNIT + lane
            for j, (scores, dp) in enumerate(out):
                key_block = slots[j] * NY + y
                key_len = count_ref[key_block] * UNIT
                most = jnp.where(query_block > key_block, CAP, -1)
                limit = jnp.where(query_block == key_block, row_in, most)
                limit = jnp.where(row_in < query_len, jnp.minimum(limit, key_len - 1), -1)
                prob = jnp.exp2(scores * (SCALE * LOG2E) - norm)
                prob = jnp.where(key <= limit, prob, 0.0)
                db[i % 2, j] = (prob * (dp - delta)).astype(BF16)
                pb[i % 2, j] = prob.astype(BF16)

        def grads(i):
            qn, gn = operands(i)
            for j, slot in enumerate(slots):
                for p, (left, right) in enumerate(((db, qn), (pb, gn))):
                    total = dot(left[i % 2, j], right, ((1,), (0,)))
                    acc[slot, p] = total if fresh and i == 0 else acc[slot, p] + total
            b, u = units[i]
            total = dot(kt[slots[0]], db[i % 2, 0], ((1,), (0,)))
            for j in range(1, len(slots)):
                total = total + dot(kt[slots[j]], db[i % 2, j], ((1,), (0,)))
            dqt[b, u] += total

        weights(0, products(0))
        for i in range(1, len(units)):
            out = products(i)
            grads(i - 1)
            weights(i, out)
        grads(len(units) - 1)

    def pair(row, g):
        if isinstance(g, int):
            return [(row, g), (row, -g if g else 4)]
        return [(row, g), (row, 4 * (1 - (g + 3) // 4) - g)]

    for s in range(1, 3):
        for d in range(2):
            for p in range(2):
                ring(d, p, s - 1).wait_recv()
                ring(d, p, s).start()
                if s == 1:
                    @pl.when(x == 0)
                    def _():
                        cross(CROSS.index(-DIRS[d]), p).start()
        if s == 2:
            side(0, 0).wait_recv()
            far_side(0, 0).start()
            side(0, 2).wait_recv()
            far_side(0, 2).start()
        block(pair(x, s), [y], True)

    @pl.when(x == 1)
    def _():
        for d in range(2):
            for p in range(2):
                crossed(CROSS.index(-DIRS[d]), p).wait_recv()
                extra(d, p, 1).start()

    for d in range(2):
        for p in range(2):
            ring(d, p, 2).wait_recv()
            if valid(d, p, 3):
                ring(d, p, 3).start()
    side(1, 1).wait_recv()
    far_side(1, 1).start()
    block(pair(x, 3), [y], True)

    @pl.when(x == 1)
    def _():
        for d in range(2):
            for p in range(2):
                extra(d, p, 1).wait_recv()
                extra(d, p, 2).start()
        block(pair(0, 1), [y], True)

    for p in range(2):
        ring(p, p, 3).wait_recv()
    block(pair(x, 0), [y], True)

    @pl.when(x == 1)
    def _():
        for d in range(2):
            for p in range(2):
                extra(d, p, 2).wait_recv()
                if valid(d, p, 3):
                    extra(d, p, 3).start()
        for p in range(2):
            crossed(0, p).wait_recv()

        @pl.loop(2, 4)
        def _(g):
            block(pair(0, g), [y], True)

    side(1, 0).wait_recv()
    side(0, 1).wait_recv()
    side(1, 2).wait_recv()
    for d, a in ((0, 0), (1, 1), (0, 2)):
        far_side(d, a).wait_recv()

    copies = weight_copies((wq, wk, wv), wbuf, wsem, 0)

    @pl.when(x == 1)
    def _():
        for p in range(2):
            extra(p, p, 3).wait_recv()
        block(pair(0, 0), [y], True)

    @pl.loop(0, 4 * (1 + x))
    def _(t):
        block(pair(x * (1 - t // 4), lax.rem(t, 4)), [yy(2)], False)

    tall = fst.shape[0]
    parts = (slice(0, tall // 2), slice(tall // 2, tall))

    def far_grad(d):
        return move(fst.at[parts[d]], frb.at[parts[d]], sy.at[0, 0, d], sy.at[0, 1, d], along_y(d))

    def side_grad(d):
        return move(yst.at[d], yrb.at[d], sy.at[1, 0, d], sy.at[1, 1, d], along_y(d))

    def query_grad(b):
        return jnp.concatenate([dqt[b, u] * SCALE for u in range(UNITS)], axis=0)

    fst[...] = query_grad(yy(2)).astype(BF16)
    for d in range(2):
        far_grad(d).start()

    def sum_ring(d, p, s):
        return move(zst.at[d, p, s], zrb.at[d, p, s], sz.at[0, 0, d, p, s], sz.at[0, 1, d, p, s], along_z(d))

    def sum_extra(d, p, s):
        return move(est.at[d, p, s], erb.at[d, p, s], sz.at[1, 0, d, p, s], sz.at[1, 1, d, p, s], along_z(d))

    def sum_cross(i, p):
        return move(xst.at[i, p], xrb.at[i, p], sx.at[0, i, p], sx.at[1, i, p], twin)

    def term(row, e, p):
        value = acc[row * NZ + zz(e), p]
        return value * SCALE if p == 0 else value

    def starts(d, p, s):
        return s > 0 or d == p

    def both_ways(row, level):
        ends = (level,) if level in (0, 4) else (level, -level)
        block([(row, e) for e in ends], [yy(1), yy(-1)], False)

    for s in range(4):
        far_off = 4 - s

        @pl.when(x == 1)
        def _():
            both_ways(0, far_off)
            for d in range(2):
                for p in range(2):
                    e = DIRS[d] * far_off
                    if not starts(d, p, s):
                        continue
                    value = term(0, e, p)
                    if s in (1, 2) and starts(d, p, s - 1):
                        sum_extra(d, p, s - 1).wait_recv()
                        value = value + erb[d, p, s - 1].astype(F32)
                    if s < 2:
                        est[d, p, s] = value.astype(BF16)
                        sum_extra(d, p, s).start()
                    else:
                        xst[CROSS.index(e), p] = value.astype(BF16)
                        sum_cross(CROSS.index(e), p).start()

        both_ways(x, far_off)
        for d in range(2):
            for p in range(2):
                if not starts(d, p, s):
                    continue
                value = term(x, DIRS[d] * far_off, p)
                if s > 0 and starts(d, p, s - 1):
                    sum_ring(d, p, s - 1).wait_recv()
                    value = value + zrb[d, p, s - 1].astype(F32)
                zst[d, p, s] = value.astype(BF16)
                if s >= 2:
                    @pl.when(x == 0)
                    def _():
                        i = CROSS.index(DIRS[d] * far_off)
                        sum_cross(i, p).wait_recv()
                        zst[d, p, s] = (value + xrb[i, p].astype(F32)).astype(BF16)
                sum_ring(d, p, s).start()

    @pl.when(x == 1)
    def _():
        both_ways(0, 0)
        for p in range(2):
            xst[0, p] = term(0, 0, p).astype(BF16)
            sum_cross(0, p).start()

    both_ways(x, 0)
    for d in range(2):
        far_grad(d).wait_recv()
        value = query_grad(yy(DIRS[d]))
        yst[d] = value.astype(BF16)
        yst[d, parts[d]] = (value[parts[d]] + frb[parts[d]].astype(F32)).astype(BF16)
        side_grad(d).start()
    for group in copies:
        for copy in group:
            copy.wait()

    outs = (dk_out, dv_out)
    row_of = lax.broadcasted_iota(jnp.int32, (CAP, HD), 0)
    for p in range(2):
        value = term(x, 0, p)
        for d in range(2):
            sum_ring(d, p, 3).wait_recv()
            value = value + zrb[d, p, 3].astype(F32)
        outs[p][...] = value

        @pl.when(x == 0)
        def _():
            sum_cross(0, p).wait_recv()
            outs[p][...] = value + xrb[0, p].astype(F32)

        act[:, (GROUP + p) * HD:(GROUP + p + 1) * HD] = outs[p][...].astype(BF16)

    value = query_grad(y)
    for d in range(2):
        side_grad(d).wait_recv()
        value = value + yrb[d].astype(F32)
    for u in range(UNITS):
        turned = value[u * HD:(u + 1) * HD].T.astype(BF16)
        for h in range(GROUP):
            act[u * UNIT:(u + 1) * UNIT, h * HD:(h + 1) * HD] = turned[h * UNIT:(h + 1) * UNIT]

    def columns(c):
        return pl.ds(pl.multiple_of(c * width, width), width)

    height = CAP // PIECES
    rows = [pl.ds(i * height, height) for i in range(PIECES)]

    def swap(i, which):
        src, dst = ((far, farb), (near, nearb))[which]
        return move(
            src.at[rows[i], columns(1 - core)], dst.at[rows[i]], hs.at[which, 0, i], hs.at[which, 1, i], partner
        )

    def hop(i):
        return move(stage.at[rows[i]], relay.at[rows[i]], hs.at[2, 0, i], hs.at[2, 1, i], device(DIRS[i % 2]))

    def forward(i):
        return move(relay.at[rows[i]], last.at[rows[i]], hs.at[3, 0, i], hs.at[3, 1, i], device(DIRS[i % 2]))

    def product(c):
        return dot(act[...], wbuf[c], ((1,), (1,))).astype(BF16)

    for c in range(tiles):
        far[:, c * TILE:(c + 1) * TILE] = product((1 - x_hi) * tiles + c)
    for i in range(PIECES):
        swap(i, 0).start()
    for i in range(PIECES):
        swap(i, 0).wait_recv()
        mine = far[rows[i], columns(core)].astype(F32)
        stage[rows[i]] = (mine + farb[rows[i]].astype(F32)).astype(BF16)
        hop(i).start()
    for c in range(tiles):
        near[:, c * TILE:(c + 1) * TILE] = product(x_hi * tiles + c)
    for i in range(PIECES):
        swap(i, 1).start()
    for i in range(PIECES):
        hop(i).wait_recv()
        forward(i).start()
    for i in range(PIECES):
        swap(i, 1).wait_recv()
        forward(i).wait_recv()
        mine = near[rows[i], columns(core)].astype(F32)
        total = mine + nearb[rows[i]].astype(F32) + last[rows[i]].astype(F32)
        out_ref[rows[i]] = total.astype(BF16)

    for d in range(2):
        for p in range(2):
            for s in range(4):
                if valid(d, p, s):
                    ring(d, p, s).wait_send()
                if starts(d, p, s):
                    sum_ring(d, p, s).wait_send()
        for a in range(3):
            side(d, a).wait_send()
        far_grad(d).wait_send()
        side_grad(d).wait_send()
    for d, a in ((0, 0), (1, 1), (0, 2)):
        far_side(d, a).wait_send()

    @pl.when(x == 0)
    def _():
        for p in range(2):
            for i in range(3):
                cross(i, p).wait_send()

    @pl.when(x == 1)
    def _():
        for p in range(2):
            for d in range(2):
                for s in range(1, 4):
                    if valid(d, p, s):
                        extra(d, p, s).wait_send()
                for s in range(2):
                    if starts(d, p, s):
                        sum_extra(d, p, s).wait_send()
            for i in range(5):
                sum_cross(i, p).wait_send()

    for i in range(PIECES):
        for which in range(2):
            swap(i, which).wait_send()
        hop(i).wait_send()
        forward(i).wait_send()


def on_device(q, k, v, o, g, lse, counts, wq, wk, wv):
    dma = pltpu.SemaphoreType.DMA
    hbm = pl.BlockSpec(memory_space=pl.ANY)
    blocks, units = NX * NZ, CAP // UNIT
    model = wq.shape[0]
    features = wq.shape[1] + wk.shape[1] + wv.shape[1]
    tile = (CAP, HD)
    flat = (units * HD, GROUP * UNIT)
    quarter = (CAP, model // 4)

    def vmem(shape, dtype=BF16):
        return pltpu.VMEM(shape, dtype)

    return pl.pallas_call(
        fused_kernel,
        name="attention_backward",
        out_shape=(
            jax.ShapeDtypeStruct(quarter, BF16),
            jax.ShapeDtypeStruct(tile, F32),
            jax.ShapeDtypeStruct(tile, F32),
        ),
        in_specs=[SMEM] + [VMEM] * 6 + [hbm] * 3,
        out_specs=(VMEM,) * 3,
        scratch_shapes=[
            vmem((blocks, 2) + tile),
            vmem((NY, CAP, GROUP * HD)),
            vmem((NY, CAP, GROUP * HD)),
            vmem((NY, 8, GROUP * UNIT), F32),
            vmem((blocks, HD, CAP)),
            vmem((blocks, 2) + tile, F32),
            vmem((NY, units, HD, GROUP * UNIT), F32),
            vmem((2, 2, CAP, GROUP * UNIT)), vmem((2, 2, CAP, GROUP * UNIT)),
            vmem((2, 2, 4) + tile), vmem((2, 2, 4) + tile),
            vmem((2, 2, 2) + tile), vmem((2, 2, 2) + tile),
            vmem((5, 2) + tile), vmem((5, 2) + tile),
            vmem(flat), vmem(flat), vmem((2,) + flat), vmem((2,) + flat),
            vmem((CAP, features)),
            vmem((CAP, model // 2)), vmem((CAP, model // 2)),
            vmem(quarter), vmem(quarter), vmem(quarter), vmem(quarter), vmem(quarter),
            vmem((model // TILE, TILE, features)),
            dma((2, 2, 2, 2, 4)), dma((2, 3, 2)), dma((2, 2, 2, 3)),
            dma((2, 2, 2, 2, 4)), dma((2, 5, 2)), dma((2, 2, 2)),
            dma((4, 2, PIECES)), dma((model // TILE, 3)),
        ],
        compiler_params=pltpu.CompilerParams(collective_id=0, has_side_effects=True),
    )(counts, k, v, q, g, o, lse, wq, wk, wv)


def solution(mesh):
    return jax.shard_map(
        on_device,
        mesh=mesh,
        in_specs=(
            P("ctx", "heads"), P("ctx", "heads"), P("ctx", "heads"), P("ctx", "heads"), P("ctx", "heads"),
            P("heads", "ctx"), P(), P(None, "heads"), P(None, "heads"), P(None, "heads"),
        ),
        out_specs=(P("ctx", "heads"), P("ctx", "heads"), P("ctx", "heads")),
        check_vma=False,
    )
```

```python
import math

import jax
import jax.numpy as jnp
from jax import lax
from jax.experimental import pallas as pl
from jax.experimental.pallas import tpu as pltpu
from jax.sharding import PartitionSpec as P

UNIT = 64
CAP = 192
HD = 128
GROUP = 4
NX, NZ, NY = 2, 8, 4
TILE = 256
PIECES = 6
LOG2E = math.log2(math.e)
SCALE = 1.0 / math.sqrt(HD)
MESH = pl.DeviceIdType.MESH
VMEM = pl.BlockSpec(memory_space=pltpu.VMEM)
SMEM = pl.BlockSpec(memory_space=pltpu.SMEM)
F32 = jnp.float32
BF16 = jnp.bfloat16


def place():
    c = lax.axis_index("ctx")
    return c // (NZ * NY), lax.rem(c // NY, NZ), lax.rem(c, NY)


def ctx_id(x, z, y):
    return {"ctx": (x * NZ + z) * NY + y}


def move(src, dst, send, recv, to):
    return pltpu.make_async_remote_copy(
        src_ref=src, dst_ref=dst, send_sem=send, recv_sem=recv, device_id=to, device_id_type=MESH
    )


def greet(peers):
    barrier = pltpu.get_barrier_semaphore()
    for peer in peers:
        pl.semaphore_signal(barrier, inc=1, device_id=peer, device_id_type=MESH)
    pl.semaphore_wait(barrier, len(peers))


DIRS = (1, -1)
CROSS = (0, 1, -1)


def weight_copies(w_refs, buf, sems, first):
    copies = []
    for c in range(buf.shape[0]):
        rows, at, group = pl.ds(pl.multiple_of(first + c * TILE, TILE), TILE), 0, []
        for i, w in enumerate(w_refs):
            width = w.shape[1]
            group.append(pltpu.make_async_copy(w.at[rows], buf.at[c, :, at:at + width], sems.at[c, i]))
            at += width
        copies.append(group)
    for group in copies:
        for copy in group:
            copy.start()
    return copies


def dot(a, b, dims):
    return lax.dot_general(a, b, (dims, ((), ())), preferred_element_type=F32)


def fused_kernel(
    count_ref, k_ref, v_ref, q_ref, g_ref, o_ref, lse_ref, wq, wk, wv,
    out_ref, dk_out, dv_out,
    kv, qa, ga, st, kt, acc, dqt, pb, db,
    zst, zrb, est, erb, xst, xrb, fst, frb, yst, yrb,
    act, far, near, farb, nearb, stage, relay, last, wbuf,
    gz, gx, gy, sz, sx, sy, hs, wsem,
):
    hd = lax.axis_index("heads")
    x, z, y = place()
    x_hi, core = hd // 2, lax.rem(hd, 2)
    xx = x_hi * 2 + x
    width = out_ref.shape[1]
    tiles = wbuf.shape[0] // 2
    UNITS = CAP // UNIT
    own = (k_ref, v_ref)

    def zz(k):
        return lax.rem(z + k + NZ, NZ)

    def yy(k):
        return lax.rem(y + k + NY, NY)

    def device(k):
        to = lax.rem(xx + k + 4, 4)
        return {"heads": (to // 2) * 2 + core, **ctx_id(lax.rem(to, 2), z, y)}

    partner = {"heads": x_hi * 2 + 1 - core}

    def along_z(d):
        return ctx_id(x, zz(DIRS[d]), y)

    def along_y(d):
        return ctx_id(x, z, yy(DIRS[d]))

    twin = ctx_id(1 - x, z, y)
    st[y] = jnp.zeros(st.shape[1:], F32)
    for h in range(GROUP):
        cols = slice(h * HD, (h + 1) * HD)
        both = g_ref[:, cols].astype(F32) * o_ref[:, cols].astype(F32)
        delta = jnp.sum(both.T, axis=0, keepdims=True)
        norm = lse_ref[h:h + 1, :] * LOG2E
        for u in range(UNITS):
            part = slice(u * UNIT, (u + 1) * UNIT)
            into = slice(h * UNIT, (h + 1) * UNIT)
            st[y, u:u + 1, into] = norm[:, part]
            st[y, u + 4:u + 5, into] = delta[:, part]
    greet([along_z(0), along_z(1), along_y(0), along_y(1), partner, device(1), device(-1)])

    def ring(d, p, s):
        slot = x * NZ + zz(-DIRS[d] * s)
        src = own[p] if s == 0 else kv.at[slot, p]
        return move(src, kv.at[slot, p], gz.at[0, 0, d, p, s], gz.at[0, 1, d, p, s], along_z(d))

    def extra(d, p, s):
        slot = zz(-DIRS[d] * s)
        return move(kv.at[slot, p], kv.at[slot, p], gz.at[1, 0, d, p, s], gz.at[1, 1, d, p, s], along_z(d))

    def cross(i, p):
        slot = zz(CROSS[i])
        src = own[p] if i == 0 else kv.at[slot, p]
        return move(src, kv.at[slot, p], gx.at[0, i, p], gx.at[1, i, p], twin)

    def crossed(i, p):
        slot = zz(CROSS[i])
        return move(kv.at[slot, p], kv.at[slot, p], gx.at[0, i, p], gx.at[1, i, p], twin)

    sources, targets = (q_ref, g_ref, st.at[y]), (qa, ga, st)

    def side(d, a):
        return move(sources[a], targets[a].at[y], gy.at[0, 0, d, a], gy.at[0, 1, d, a], along_y(d))

    def far_side(d, a):
        slot = yy(-DIRS[d])
        return move(
            targets[a].at[slot], targets[a].at[slot], gy.at[1, 0, d, a], gy.at[1, 1, d, a], along_y(d)
        )

    def valid(d, p, s):
        return s < 3 or d == p

    for p in range(2):
        for d in range(2):
            ring(d, p, 0).start()

    @pl.when(x == 0)
    def _():
        for p in range(2):
            cross(0, p).start()

    side(0, 2).start()
    side(1, 2).start()
    side(0, 0).start()
    side(1, 1).start()
    side(1, 0).start()
    side(0, 1).start()
    kv[x * NZ + z, 0] = k_ref[...]
    kv[x * NZ + z, 1] = v_ref[...]
    qa[y] = q_ref[...]
    ga[y] = g_ref[...]
    dqt[...] = jnp.zeros_like(dqt)

    lane = lax.rem(lax.broadcasted_iota(jnp.int32, (1, GROUP * UNIT), 1), UNIT)
    key = lax.broadcasted_iota(jnp.int32, (CAP, GROUP * UNIT), 0)
    heads = [slice(h * HD, (h + 1) * HD) for h in range(GROUP)]

    def block(keys, query_blocks, fresh):
        slots = [row * NZ + zz(e) for row, e in keys]
        units = [(b, u) for b in query_blocks for u in range(UNITS)]
        if fresh:
            for slot in slots:
                kt[slot] = kv[slot, 0].T

        def operands(i):
            b, u = units[i]
            at = slice(u * UNIT, (u + 1) * UNIT)
            qn = jnp.concatenate([qa[b, at, h] for h in heads], axis=0)
            gn = jnp.concatenate([ga[b, at, h] for h in heads], axis=0)
            return qn, gn

        def products(i):
            qn, gn = operands(i)
            return [(dot(kv[s, 0], qn, ((1,), (1,))), dot(kv[s, 1], gn, ((1,), (1,)))) for s in slots]

        def weights(i, out):
            b, u = units[i]
            norm, delta = st[b, u:u + 1, :], st[b, u + 4:u + 5, :]
            query_block = (x * NZ + z) * NY + b
            query_len = count_ref[query_block] * UNIT
            row_in = u * UNIT + lane
            for j, (scores, dp) in enumerate(out):
                key_block = slots[j] * NY + y
                key_len = count_ref[key_block] * UNIT
                most = jnp.where(query_block > key_block, CAP, -1)
                limit = jnp.where(query_block == key_block, row_in, most)
                limit = jnp.where(row_in < query_len, jnp.minimum(limit, key_len - 1), -1)
                prob = jnp.exp2(scores * (SCALE * LOG2E) - norm)
                prob = jnp.where(key <= limit, prob, 0.0)
                db[i % 2, j] = (prob * (dp - delta)).astype(BF16)
                pb[i % 2, j] = prob.astype(BF16)

        def grads(i):
            qn, gn = operands(i)
            for j, slot in enumerate(slots):
                for p, (left, right) in enumerate(((db, qn), (pb, gn))):
                    total = dot(left[i % 2, j], right, ((1,), (0,)))
                    acc[slot, p] = total if fresh and i == 0 else acc[slot, p] + total
            b, u = units[i]
            total = dot(kt[slots[0]], db[i % 2, 0], ((1,), (0,)))
            for j in range(1, len(slots)):
                total = total + dot(kt[slots[j]], db[i % 2, j], ((1,), (0,)))
            dqt[b, u] += total

        weights(0, products(0))
        for i in range(1, len(units)):
            out = products(i)
            grads(i - 1)
            weights(i, out)
        grads(len(units) - 1)

    def pair(row, g):
        if isinstance(g, int):
            return [(row, g), (row, -g if g else 4)]
        return [(row, g), (row, 4 * (1 - (g + 3) // 4) - g)]

    for s in range(1, 3):
        for p in range(2):
            for d in range(2):
                ring(d, p, s - 1).wait_recv()
                ring(d, p, s).start()
                if s == 1:
                    @pl.when(x == 0)
                    def _():
                        cross(CROSS.index(-DIRS[d]), p).start()
        if s == 2:
            side(0, 0).wait_recv()
            far_side(0, 0).start()
            side(0, 2).wait_recv()
            far_side(0, 2).start()
        block(pair(x, s), [y], True)

    @pl.when(x == 1)
    def _():
        for p in range(2):
            for d in range(2):
                crossed(CROSS.index(-DIRS[d]), p).wait_recv()
                extra(d, p, 1).start()

    for p in range(2):
        for d in range(2):
            ring(d, p, 2).wait_recv()
            if valid(d, p, 3):
                ring(d, p, 3).start()
    side(1, 1).wait_recv()
    far_side(1, 1).start()
    block(pair(x, 3), [y], True)

    @pl.when(x == 1)
    def _():
        for p in range(2):
            for d in range(2):
                extra(d, p, 1).wait_recv()
                extra(d, p, 2).start()

    side(1, 0).wait_recv()
    side(0, 1).wait_recv()
    side(1, 2).wait_recv()
    block(pair(x, 1), [yy(1), yy(-1)], False)

    @pl.when(x == 1)
    def _():
        block(pair(0, 1), [y], True)

    for p in range(2):
        ring(p, p, 3).wait_recv()
    block(pair(x, 0), [y], True)

    @pl.when(x == 1)
    def _():
        for p in range(2):
            for d in range(2):
                extra(d, p, 2).wait_recv()
                if valid(d, p, 3):
                    extra(d, p, 3).start()
        for p in range(2):
            crossed(0, p).wait_recv()

        @pl.loop(2, 4)
        def _(g):
            block(pair(0, g), [y], True)

    block([(x, 0)], [yy(1), yy(-1)], False)
    for d, a in ((0, 0), (1, 1), (0, 2)):
        far_side(d, a).wait_recv()

    copies = weight_copies((wq, wk, wv), wbuf, wsem, 0)

    @pl.when(x == 1)
    def _():
        for p in range(2):
            extra(p, p, 3).wait_recv()
        block(pair(0, 0), [y], True)

    tall = fst.shape[0]
    parts = (slice(0, tall // 2), slice(tall // 2, tall))

    def far_grad(d):
        return move(fst.at[parts[d]], frb.at[parts[d]], sy.at[0, 0, d], sy.at[0, 1, d], along_y(d))

    def side_grad(d):
        return move(yst.at[d], yrb.at[d], sy.at[1, 0, d], sy.at[1, 1, d], along_y(d))

    def query_grad(b):
        return jnp.concatenate([dqt[b, u] * SCALE for u in range(UNITS)], axis=0)

    def sum_ring(d, p, s):
        return move(zst.at[d, p, s], zrb.at[d, p, s], sz.at[0, 0, d, p, s], sz.at[0, 1, d, p, s], along_z(d))

    def sum_extra(d, p, s):
        return move(est.at[d, p, s], erb.at[d, p, s], sz.at[1, 0, d, p, s], sz.at[1, 1, d, p, s], along_z(d))

    def sum_cross(i, p):
        return move(xst.at[i, p], xrb.at[i, p], sx.at[0, i, p], sx.at[1, i, p], twin)

    def term(row, e, p):
        value = acc[row * NZ + zz(e), p]
        return value * SCALE if p == 0 else value

    def starts(d, p, s):
        return s > 0 or s == 0 and d == p

    def rest(row, level, shifts):
        ends = (level,) if level in (0, 4) else (level, -level)
        block([(row, e) for e in ends], [yy(k) for k in shifts], False)

    sides, three = (1, -1), (2, 1, -1)

    def send_first_row(s):
        for p in range(2):
            for d in range(2):
                if not starts(d, p, s):
                    continue
                value = term(0, DIRS[d] * (4 - s), p)
                if starts(d, p, s - 1):
                    sum_extra(d, p, s - 1).wait_recv()
                    value = value + erb[d, p, s - 1].astype(F32)
                if s < 3:
                    est[d, p, s] = value.astype(BF16)
                    sum_extra(d, p, s).start()
                else:
                    xst[CROSS.index(DIRS[d]), p] = value.astype(BF16)
                    sum_cross(CROSS.index(DIRS[d]), p).start()

    def send_own_row(s):
        for p in range(2):
            for d in range(2):
                if not starts(d, p, s):
                    continue
                value = term(x, DIRS[d] * (4 - s), p)
                if starts(d, p, s - 1):
                    sum_ring(d, p, s - 1).wait_recv()
                    value = value + zrb[d, p, s - 1].astype(F32)
                zst[d, p, s] = value.astype(BF16)
                if s == 3:
                    @pl.when(x == 0)
                    def _():
                        i = CROSS.index(DIRS[d])
                        sum_cross(i, p).wait_recv()
                        zst[d, p, s] = (value + xrb[i, p].astype(F32)).astype(BF16)
                sum_ring(d, p, s).start()

    @pl.when(x == 1)
    def _():
        rest(0, 4, three)
        send_first_row(0)

    rest(x, 4, three)
    send_own_row(0)

    @pl.when(x == 1)
    def _():
        rest(0, 3, three)
        send_first_row(1)

    @pl.loop(0, 2 + x)
    def _(t):
        block(pair(x * (1 - t // 2), 1 + lax.rem(t, 2)), [yy(2)], False)

    rest(x, 3, three)
    send_own_row(1)

    @pl.when(x == 1)
    def _():
        rest(0, 2, three)
        send_first_row(2)
        block([(0, 0), (1, 0)], [yy(2)], False)

    @pl.when(x == 0)
    def _():
        rest(0, 0, (2,))

    fst[...] = query_grad(yy(2)).astype(BF16)
    for d in range(2):
        far_grad(d).start()

    @pl.when(x == 1)
    def _():
        rest(0, 1, sides)

    rest(x, 2, sides)

    @pl.when(x == 1)
    def _():
        send_first_row(3)

    send_own_row(2)

    @pl.when(x == 1)
    def _():
        rest(0, 0, sides)
        for p in range(2):
            xst[0, p] = term(0, 0, p).astype(BF16)
            sum_cross(0, p).start()

    for d in range(2):
        far_grad(d).wait_recv()
        value = query_grad(yy(DIRS[d]))
        yst[d] = value.astype(BF16)
        yst[d, parts[d]] = (value[parts[d]] + frb[parts[d]].astype(F32)).astype(BF16)
        side_grad(d).start()
    send_own_row(3)
    for group in copies:
        for copy in group:
            copy.wait()

    outs = (dk_out, dv_out)
    row_of = lax.broadcasted_iota(jnp.int32, (CAP, HD), 0)
    for p in range(2):
        value = term(x, 0, p)
        for d in range(2):
            sum_ring(d, p, 3).wait_recv()
            value = value + zrb[d, p, 3].astype(F32)
        outs[p][...] = value

        @pl.when(x == 0)
        def _():
            sum_cross(0, p).wait_recv()
            outs[p][...] = value + xrb[0, p].astype(F32)

        act[:, (GROUP + p) * HD:(GROUP + p + 1) * HD] = outs[p][...].astype(BF16)

    value = query_grad(y)
    for d in range(2):
        side_grad(d).wait_recv()
        value = value + yrb[d].astype(F32)
    for u in range(UNITS):
        turned = value[u * HD:(u + 1) * HD].T.astype(BF16)
        for h in range(GROUP):
            act[u * UNIT:(u + 1) * UNIT, h * HD:(h + 1) * HD] = turned[h * UNIT:(h + 1) * UNIT]

    def columns(c):
        return pl.ds(pl.multiple_of(c * width, width), width)

    height = CAP // PIECES
    rows = [pl.ds(i * height, height) for i in range(PIECES)]

    def swap(i, which):
        src, dst = ((far, farb), (near, nearb))[which]
        return move(
            src.at[rows[i], columns(1 - core)], dst.at[rows[i]], hs.at[which, 0, i], hs.at[which, 1, i], partner
        )

    def hop(i):
        return move(stage.at[rows[i]], relay.at[rows[i]], hs.at[2, 0, i], hs.at[2, 1, i], device(DIRS[i % 2]))

    def forward(i):
        return move(relay.at[rows[i]], last.at[rows[i]], hs.at[3, 0, i], hs.at[3, 1, i], device(DIRS[i % 2]))

    def product(c):
        return dot(act[...], wbuf[c], ((1,), (1,))).astype(BF16)

    for c in range(tiles):
        far[:, c * TILE:(c + 1) * TILE] = product((1 - x_hi) * tiles + c)
    for i in range(PIECES):
        swap(i, 0).start()
    for i in range(PIECES):
        swap(i, 0).wait_recv()
        mine = far[rows[i], columns(core)].astype(F32)
        stage[rows[i]] = (mine + farb[rows[i]].astype(F32)).astype(BF16)
        hop(i).start()
    for c in range(tiles):
        near[:, c * TILE:(c + 1) * TILE] = product(x_hi * tiles + c)
    for i in range(PIECES):
        swap(i, 1).start()
    for i in range(PIECES):
        hop(i).wait_recv()
        forward(i).start()
    for i in range(PIECES):
        swap(i, 1).wait_recv()
        forward(i).wait_recv()
        mine = near[rows[i], columns(core)].astype(F32)
        total = mine + nearb[rows[i]].astype(F32) + last[rows[i]].astype(F32)
        out_ref[rows[i]] = total.astype(BF16)

    for d in range(2):
        for p in range(2):
            for s in range(4):
                if valid(d, p, s):
                    ring(d, p, s).wait_send()
                if starts(d, p, s):
                    sum_ring(d, p, s).wait_send()
        for a in range(3):
            side(d, a).wait_send()
        far_grad(d).wait_send()
        side_grad(d).wait_send()
    for d, a in ((0, 0), (1, 1), (0, 2)):
        far_side(d, a).wait_send()

    @pl.when(x == 0)
    def _():
        for p in range(2):
            for i in range(3):
                cross(i, p).wait_send()

    @pl.when(x == 1)
    def _():
        for p in range(2):
            for d in range(2):
                for s in range(1, 4):
                    if valid(d, p, s):
                        extra(d, p, s).wait_send()
                for s in range(3):
                    if starts(d, p, s):
                        sum_extra(d, p, s).wait_send()
            for i in range(3):
                sum_cross(i, p).wait_send()

    for i in range(PIECES):
        for which in range(2):
            swap(i, which).wait_send()
        hop(i).wait_send()
        forward(i).wait_send()


def hand_over(*refs):
    for i in range(3):
        refs[i + 3][...] = refs[i][...]


def on_device(q, k, v, o, g, lse, counts, wq, wk, wv):
    dma = pltpu.SemaphoreType.DMA
    hbm = pl.BlockSpec(memory_space=pl.ANY)
    blocks, units = NX * NZ, CAP // UNIT
    model = wq.shape[0]
    features = wq.shape[1] + wk.shape[1] + wv.shape[1]
    tile = (CAP, HD)
    flat = (units * HD, GROUP * UNIT)
    quarter = (CAP, model // 4)

    def vmem(shape, dtype=BF16):
        return pltpu.VMEM(shape, dtype)

    outs = pl.pallas_call(
        fused_kernel,
        name="attention_backward",
        out_shape=(
            jax.ShapeDtypeStruct(quarter, BF16),
            jax.ShapeDtypeStruct(tile, F32),
            jax.ShapeDtypeStruct(tile, F32),
        ),
        in_specs=[SMEM] + [VMEM] * 6 + [hbm] * 3,
        out_specs=(VMEM,) * 3,
        scratch_shapes=[
            vmem((blocks, 2) + tile),
            vmem((NY, CAP, GROUP * HD)),
            vmem((NY, CAP, GROUP * HD)),
            vmem((NY, 8, GROUP * UNIT), F32),
            vmem((blocks, HD, CAP)),
            vmem((blocks, 2) + tile, F32),
            vmem((NY, units, HD, GROUP * UNIT), F32),
            vmem((2, 2, CAP, GROUP * UNIT)), vmem((2, 2, CAP, GROUP * UNIT)),
            vmem((2, 2, 4) + tile), vmem((2, 2, 4) + tile),
            vmem((2, 2, 3) + tile), vmem((2, 2, 3) + tile),
            vmem((3, 2) + tile), vmem((3, 2) + tile),
            vmem(flat), vmem(flat), vmem((2,) + flat), vmem((2,) + flat),
            vmem((CAP, features)),
            vmem((CAP, model // 2)), vmem((CAP, model // 2)),
            vmem(quarter), vmem(quarter), vmem(quarter), vmem(quarter), vmem(quarter),
            vmem((model // TILE, TILE, features)),
            dma((2, 2, 2, 2, 4)), dma((2, 3, 2)), dma((2, 2, 2, 3)),
            dma((2, 2, 2, 2, 4)), dma((2, 3, 2)), dma((2, 2, 2)),
            dma((4, 2, PIECES)), dma((model // TILE, 3)),
        ],
        compiler_params=pltpu.CompilerParams(collective_id=0, has_side_effects=True),
    )(counts, k, v, q, g, o, lse, wq, wk, wv)
    return pl.pallas_call(
        hand_over,
        name="hand_over",
        out_shape=tuple(jax.ShapeDtypeStruct(a.shape, a.dtype) for a in outs),
        in_specs=[VMEM] * 3,
        out_specs=(VMEM,) * 3,
    )(*outs)


def solution(mesh):
    return jax.shard_map(
        on_device,
        mesh=mesh,
        in_specs=(
            P("ctx", "heads"), P("ctx", "heads"), P("ctx", "heads"), P("ctx", "heads"), P("ctx", "heads"),
            P("heads", "ctx"), P(), P(None, "heads"), P(None, "heads"), P(None, "heads"),
        ),
        out_specs=(P("ctx", "heads"), P("ctx", "heads"), P("ctx", "heads")),
        check_vma=False,
    )
```

```python
import math

import jax
import jax.numpy as jnp
from jax import lax
from jax.experimental import pallas as pl
from jax.experimental.pallas import tpu as pltpu
from jax.sharding import PartitionSpec as P

UNIT = 64
CAP = 192
HD = 128
GROUP = 4
NX, NZ, NY = 2, 8, 4
TILE = 256
PIECES = 6
LOG2E = math.log2(math.e)
SCALE = 1.0 / math.sqrt(HD)
MESH = pl.DeviceIdType.MESH
VMEM = pl.BlockSpec(memory_space=pltpu.VMEM)
SMEM = pl.BlockSpec(memory_space=pltpu.SMEM)
F32 = jnp.float32
BF16 = jnp.bfloat16


def place():
    c = lax.axis_index("ctx")
    return c // (NZ * NY), lax.rem(c // NY, NZ), lax.rem(c, NY)


def ctx_id(x, z, y):
    return {"ctx": (x * NZ + z) * NY + y}


def move(src, dst, send, recv, to):
    return pltpu.make_async_remote_copy(
        src_ref=src, dst_ref=dst, send_sem=send, recv_sem=recv, device_id=to, device_id_type=MESH
    )


def greet(peers):
    barrier = pltpu.get_barrier_semaphore()
    for peer in peers:
        pl.semaphore_signal(barrier, inc=1, device_id=peer, device_id_type=MESH)
    pl.semaphore_wait(barrier, len(peers))


DIRS = (1, -1)
CROSS = (0, 1, -1)


def weight_copies(w_refs, buf, sems, first):
    copies = []
    for c in range(buf.shape[0]):
        rows, at, group = pl.ds(pl.multiple_of(first + c * TILE, TILE), TILE), 0, []
        for i, w in enumerate(w_refs):
            width = w.shape[1]
            group.append(pltpu.make_async_copy(w.at[rows], buf.at[c, :, at:at + width], sems.at[c, i]))
            at += width
        copies.append(group)
    for group in copies:
        for copy in group:
            copy.start()
    return copies


def dot(a, b, dims):
    return lax.dot_general(a, b, (dims, ((), ())), preferred_element_type=F32)


def fused_kernel(
    count_ref, k_ref, v_ref, q_ref, g_ref, o_ref, lse_ref, wq, wk, wv,
    out_ref, dk_out, dv_out,
    kv, qa, ga, st, kt, acc, dqt, pb, db,
    zst, zrb, est, erb, xst, xrb, fst, frb, yst, yrb,
    act, far, near, farb, nearb, stage, relay, last, wbuf,
    gz, gx, gy, sz, sx, sy, hs, wsem,
):
    hd = lax.axis_index("heads")
    x, z, y = place()
    x_hi, core = hd // 2, lax.rem(hd, 2)
    xx = x_hi * 2 + x
    width = out_ref.shape[1]
    tiles = wbuf.shape[0] // 2
    UNITS = CAP // UNIT
    own = (k_ref, v_ref)

    def zz(k):
        return lax.rem(z + k + NZ, NZ)

    def yy(k):
        return lax.rem(y + k + NY, NY)

    def device(k):
        to = lax.rem(xx + k + 4, 4)
        return {"heads": (to // 2) * 2 + core, **ctx_id(lax.rem(to, 2), z, y)}

    partner = {"heads": x_hi * 2 + 1 - core}

    def along_z(d):
        return ctx_id(x, zz(DIRS[d]), y)

    def along_y(d):
        return ctx_id(x, z, yy(DIRS[d]))

    twin = ctx_id(1 - x, z, y)
    st[y] = jnp.zeros(st.shape[1:], F32)
    for h in range(GROUP):
        cols = slice(h * HD, (h + 1) * HD)
        both = g_ref[:, cols].astype(F32) * o_ref[:, cols].astype(F32)
        delta = jnp.sum(both.T, axis=0, keepdims=True)
        norm = lse_ref[h:h + 1, :] * LOG2E
        for u in range(UNITS):
            part = slice(u * UNIT, (u + 1) * UNIT)
            into = slice(h * UNIT, (h + 1) * UNIT)
            st[y, u:u + 1, into] = norm[:, part]
            st[y, u + 4:u + 5, into] = delta[:, part]
    greet([along_z(0), along_z(1), along_y(0), along_y(1), partner, device(1), device(-1)])

    def ring(d, p, s):
        slot = x * NZ + zz(-DIRS[d] * s)
        src = own[p] if s == 0 else kv.at[slot, p]
        return move(src, kv.at[slot, p], gz.at[0, 0, d, p, s], gz.at[0, 1, d, p, s], along_z(d))

    def extra(d, p, s):
        slot = zz(-DIRS[d] * s)
        return move(kv.at[slot, p], kv.at[slot, p], gz.at[1, 0, d, p, s], gz.at[1, 1, d, p, s], along_z(d))

    def cross(i, p):
        slot = zz(CROSS[i])
        src = own[p] if i == 0 else kv.at[slot, p]
        return move(src, kv.at[slot, p], gx.at[0, i, p], gx.at[1, i, p], twin)

    def crossed(i, p):
        slot = zz(CROSS[i])
        return move(kv.at[slot, p], kv.at[slot, p], gx.at[0, i, p], gx.at[1, i, p], twin)

    sources, targets = (q_ref, g_ref, st.at[y]), (qa, ga, st)

    def side(d, a):
        return move(sources[a], targets[a].at[y], gy.at[0, 0, d, a], gy.at[0, 1, d, a], along_y(d))

    def far_side(d, a):
        slot = yy(-DIRS[d])
        return move(
            targets[a].at[slot], targets[a].at[slot], gy.at[1, 0, d, a], gy.at[1, 1, d, a], along_y(d)
        )

    def valid(d, p, s):
        return s < 3 or d == p

    for p in range(2):
        for d in range(2):
            ring(d, p, 0).start()

    @pl.when(x == 0)
    def _():
        for p in range(2):
            cross(0, p).start()

    side(0, 2).start()
    side(1, 2).start()
    side(0, 0).start()
    side(1, 1).start()
    side(1, 0).start()
    side(0, 1).start()
    kv[x * NZ + z, 0] = k_ref[...]
    kv[x * NZ + z, 1] = v_ref[...]
    qa[y] = q_ref[...]
    ga[y] = g_ref[...]
    dqt[...] = jnp.zeros_like(dqt)

    lane = lax.rem(lax.broadcasted_iota(jnp.int32, (1, GROUP * UNIT), 1), UNIT)
    key = lax.broadcasted_iota(jnp.int32, (CAP, GROUP * UNIT), 0)
    heads = [slice(h * HD, (h + 1) * HD) for h in range(GROUP)]

    def block(keys, query_blocks, fresh):
        slots = [row * NZ + zz(e) for row, e in keys]
        units = [(b, u) for b in query_blocks for u in range(UNITS)]
        if fresh:
            for slot in slots:
                kt[slot] = kv[slot, 0].T

        def operands(i):
            b, u = units[i]
            at = slice(u * UNIT, (u + 1) * UNIT)
            qn = jnp.concatenate([qa[b, at, h] for h in heads], axis=0)
            gn = jnp.concatenate([ga[b, at, h] for h in heads], axis=0)
            return qn, gn

        def products(i):
            qn, gn = operands(i)
            return [(dot(kv[s, 0], qn, ((1,), (1,))), dot(kv[s, 1], gn, ((1,), (1,)))) for s in slots]

        def weights(i, out):
            b, u = units[i]
            norm, delta = st[b, u:u + 1, :], st[b, u + 4:u + 5, :]
            query_block = (x * NZ + z) * NY + b
            query_len = count_ref[query_block] * UNIT
            row_in = u * UNIT + lane
            for j, (scores, dp) in enumerate(out):
                key_block = slots[j] * NY + y
                key_len = count_ref[key_block] * UNIT
                most = jnp.where(query_block > key_block, CAP, -1)
                limit = jnp.where(query_block == key_block, row_in, most)
                limit = jnp.where(row_in < query_len, jnp.minimum(limit, key_len - 1), -1)
                prob = jnp.exp2(scores * (SCALE * LOG2E) - norm)
                prob = jnp.where(key <= limit, prob, 0.0)
                db[i % 2, j] = (prob * (dp - delta)).astype(BF16)
                pb[i % 2, j] = prob.astype(BF16)

        def grads(i):
            qn, gn = operands(i)
            for j, slot in enumerate(slots):
                for p, (left, right) in enumerate(((db, qn), (pb, gn))):
                    total = dot(left[i % 2, j], right, ((1,), (0,)))
                    acc[slot, p] = total if fresh and i == 0 else acc[slot, p] + total
            b, u = units[i]
            total = dot(kt[slots[0]], db[i % 2, 0], ((1,), (0,)))
            for j in range(1, len(slots)):
                total = total + dot(kt[slots[j]], db[i % 2, j], ((1,), (0,)))
            dqt[b, u] += total

        weights(0, products(0))
        for i in range(1, len(units)):
            out = products(i)
            grads(i - 1)
            weights(i, out)
        grads(len(units) - 1)

    def pair(row, g):
        if isinstance(g, int):
            return [(row, g), (row, -g if g else 4)]
        return [(row, g), (row, 4 * (1 - (g + 3) // 4) - g)]

    for s in range(1, 3):
        for p in range(2):
            for d in range(2):
                ring(d, p, s - 1).wait_recv()
                ring(d, p, s).start()
                if s == 1:
                    @pl.when(x == 0)
                    def _():
                        cross(CROSS.index(-DIRS[d]), p).start()
        block(pair(x, s), [y], True)

    @pl.when(x == 1)
    def _():
        for p in range(2):
            for d in range(2):
                crossed(CROSS.index(-DIRS[d]), p).wait_recv()
                extra(d, p, 1).start()

    side(0, 0).wait_recv()
    far_side(0, 0).start()
    side(0, 2).wait_recv()
    far_side(0, 2).start()
    for p in range(2):
        for d in range(2):
            ring(d, p, 2).wait_recv()
            if valid(d, p, 3):
                ring(d, p, 3).start()
    side(1, 1).wait_recv()
    far_side(1, 1).start()
    block(pair(x, 3), [y], True)

    @pl.when(x == 1)
    def _():
        for p in range(2):
            for d in range(2):
                extra(d, p, 1).wait_recv()
                extra(d, p, 2).start()

    side(1, 0).wait_recv()
    side(0, 1).wait_recv()
    side(1, 2).wait_recv()
    block(pair(x, 1), [yy(1), yy(-1)], False)

    @pl.when(x == 1)
    def _():
        block(pair(0, 1), [y], True)

    for p in range(2):
        ring(p, p, 3).wait_recv()
    block(pair(x, 0), [y], True)

    @pl.when(x == 1)
    def _():
        for p in range(2):
            for d in range(2):
                extra(d, p, 2).wait_recv()
                if valid(d, p, 3):
                    extra(d, p, 3).start()
        for p in range(2):
            crossed(0, p).wait_recv()

        @pl.loop(2, 4)
        def _(g):
            block(pair(0, g), [y], True)

    block([(x, 0)], [yy(1), yy(-1)], False)
    for d, a in ((0, 0), (1, 1), (0, 2)):
        far_side(d, a).wait_recv()

    copies = weight_copies((wq, wk, wv), wbuf, wsem, 0)

    @pl.when(x == 1)
    def _():
        for p in range(2):
            extra(p, p, 3).wait_recv()
        block(pair(0, 0), [y], True)

    tall = fst.shape[0]
    parts = (slice(0, tall // 2), slice(tall // 2, tall))

    def far_grad(d):
        return move(fst.at[parts[d]], frb.at[parts[d]], sy.at[0, 0, d], sy.at[0, 1, d], along_y(d))

    def side_grad(d):
        return move(yst.at[d], yrb.at[d], sy.at[1, 0, d], sy.at[1, 1, d], along_y(d))

    def query_grad(b):
        return jnp.concatenate([dqt[b, u] * SCALE for u in range(UNITS)], axis=0)

    def sum_ring(d, p, s):
        return move(zst.at[d, p, s], zrb.at[d, p, s], sz.at[0, 0, d, p, s], sz.at[0, 1, d, p, s], along_z(d))

    def sum_extra(d, p, s):
        return move(est.at[d, p, s], erb.at[d, p, s], sz.at[1, 0, d, p, s], sz.at[1, 1, d, p, s], along_z(d))

    def sum_cross(i, p):
        return move(xst.at[i, p], xrb.at[i, p], sx.at[0, i, p], sx.at[1, i, p], twin)

    def term(row, e, p):
        value = acc[row * NZ + zz(e), p]
        return value * SCALE if p == 0 else value

    def starts(d, p, s):
        return s > 0 or s == 0 and d == p

    def rest(row, level, shifts):
        ends = (level,) if level in (0, 4) else (level, -level)
        block([(row, e) for e in ends], [yy(k) for k in shifts], False)

    sides, three = (1, -1), (2, 1, -1)

    def send_first_row(s):
        for p in range(2):
            for d in range(2):
                if not starts(d, p, s):
                    continue
                value = term(0, DIRS[d] * (4 - s), p)
                if starts(d, p, s - 1):
                    sum_extra(d, p, s - 1).wait_recv()
                    value = value + erb[d, p, s - 1].astype(F32)
                if s < 3:
                    est[d, p, s] = value.astype(BF16)
                    sum_extra(d, p, s).start()
                else:
                    xst[CROSS.index(DIRS[d]), p] = value.astype(BF16)
                    sum_cross(CROSS.index(DIRS[d]), p).start()

    def send_own_row(s):
        for p in range(2):
            for d in range(2):
                if not starts(d, p, s):
                    continue
                value = term(x, DIRS[d] * (4 - s), p)
                if starts(d, p, s - 1):
                    sum_ring(d, p, s - 1).wait_recv()
                    value = value + zrb[d, p, s - 1].astype(F32)
                zst[d, p, s] = value.astype(BF16)
                if s == 3:
                    @pl.when(x == 0)
                    def _():
                        i = CROSS.index(DIRS[d])
                        sum_cross(i, p).wait_recv()
                        zst[d, p, s] = (value + xrb[i, p].astype(F32)).astype(BF16)
                sum_ring(d, p, s).start()

    @pl.when(x == 1)
    def _():
        rest(0, 4, three)
        send_first_row(0)

    rest(x, 4, three)
    send_own_row(0)

    @pl.when(x == 1)
    def _():
        rest(0, 3, three)
        send_first_row(1)

    @pl.loop(0, 2 + x)
    def _(t):
        block(pair(x * (1 - t // 2), 1 + lax.rem(t, 2)), [yy(2)], False)

    @pl.when(x == 1)
    def _():
        rest(0, 2, three)
        send_first_row(2)

    rest(x, 3, three)
    send_own_row(1)

    @pl.when(x == 1)
    def _():
        block([(0, 0), (1, 0)], [yy(2)], False)

    @pl.when(x == 0)
    def _():
        rest(0, 0, (2,))

    fst[...] = query_grad(yy(2)).astype(BF16)
    for d in range(2):
        far_grad(d).start()

    @pl.when(x == 1)
    def _():
        rest(0, 1, sides)
        send_first_row(3)

    rest(x, 2, sides)
    send_own_row(2)

    @pl.when(x == 1)
    def _():
        rest(0, 0, sides)
        for p in range(2):
            xst[0, p] = term(0, 0, p).astype(BF16)
            sum_cross(0, p).start()

    for d in range(2):
        far_grad(d).wait_recv()
        value = query_grad(yy(DIRS[d]))
        yst[d] = value.astype(BF16)
        yst[d, parts[d]] = (value[parts[d]] + frb[parts[d]].astype(F32)).astype(BF16)
        side_grad(d).start()
    send_own_row(3)
    for group in copies:
        for copy in group:
            copy.wait()

    outs = (dk_out, dv_out)
    row_of = lax.broadcasted_iota(jnp.int32, (CAP, HD), 0)
    for p in range(2):
        value = term(x, 0, p)
        for d in range(2):
            sum_ring(d, p, 3).wait_recv()
            value = value + zrb[d, p, 3].astype(F32)
        outs[p][...] = value

        @pl.when(x == 0)
        def _():
            sum_cross(0, p).wait_recv()
            outs[p][...] = value + xrb[0, p].astype(F32)

        act[:, (GROUP + p) * HD:(GROUP + p + 1) * HD] = outs[p][...].astype(BF16)

    value = query_grad(y)
    for d in range(2):
        side_grad(d).wait_recv()
        value = value + yrb[d].astype(F32)
    for u in range(UNITS):
        turned = value[u * HD:(u + 1) * HD].T.astype(BF16)
        for h in range(GROUP):
            act[u * UNIT:(u + 1) * UNIT, h * HD:(h + 1) * HD] = turned[h * UNIT:(h + 1) * UNIT]

    def columns(c):
        return pl.ds(pl.multiple_of(c * width, width), width)

    height = CAP // PIECES
    rows = [pl.ds(i * height, height) for i in range(PIECES)]

    def swap(i, which):
        src, dst = ((far, farb), (near, nearb))[which]
        return move(
            src.at[rows[i], columns(1 - core)], dst.at[rows[i]], hs.at[which, 0, i], hs.at[which, 1, i], partner
        )

    def hop(i):
        return move(stage.at[rows[i]], relay.at[rows[i]], hs.at[2, 0, i], hs.at[2, 1, i], device(DIRS[i % 2]))

    def forward(i):
        return move(relay.at[rows[i]], last.at[rows[i]], hs.at[3, 0, i], hs.at[3, 1, i], device(DIRS[i % 2]))

    def product(into, hi, c):
        at = pl.ds(pl.multiple_of(c * TILE, TILE), TILE)
        into[:, at] = dot(act[...], wbuf[hi * tiles + c], ((1,), (1,))).astype(BF16)

    for c in range(tiles // 2):
        product(far, 1 - x_hi, (1 - core) * (tiles // 2) + c)
    for i in range(PIECES):
        swap(i, 0).start()
    for c in range(tiles // 2):
        product(far, 1 - x_hi, core * (tiles // 2) + c)
    for i in range(PIECES):
        swap(i, 0).wait_recv()
        mine = far[rows[i], columns(core)].astype(F32)
        stage[rows[i]] = (mine + farb[rows[i]].astype(F32)).astype(BF16)
        hop(i).start()
    for c in range(tiles // 2):
        product(near, x_hi, (1 - core) * (tiles // 2) + c)
    for i in range(PIECES):
        swap(i, 1).start()
    for c in range(tiles // 2):
        product(near, x_hi, core * (tiles // 2) + c)
    for i in range(PIECES):
        hop(i).wait_recv()
        forward(i).start()
    for i in range(PIECES):
        swap(i, 1).wait_recv()
        forward(i).wait_recv()
        mine = near[rows[i], columns(core)].astype(F32)
        total = mine + nearb[rows[i]].astype(F32) + last[rows[i]].astype(F32)
        out_ref[rows[i]] = total.astype(BF16)

    for d in range(2):
        for p in range(2):
            for s in range(4):
                if valid(d, p, s):
                    ring(d, p, s).wait_send()
                if starts(d, p, s):
                    sum_ring(d, p, s).wait_send()
        for a in range(3):
            side(d, a).wait_send()
        far_grad(d).wait_send()
        side_grad(d).wait_send()
    for d, a in ((0, 0), (1, 1), (0, 2)):
        far_side(d, a).wait_send()

    @pl.when(x == 0)
    def _():
        for p in range(2):
            for i in range(3):
                cross(i, p).wait_send()

    @pl.when(x == 1)
    def _():
        for p in range(2):
            for d in range(2):
                for s in range(1, 4):
                    if valid(d, p, s):
                        extra(d, p, s).wait_send()
                for s in range(3):
                    if starts(d, p, s):
                        sum_extra(d, p, s).wait_send()
            for i in range(3):
                sum_cross(i, p).wait_send()

    for i in range(PIECES):
        for which in range(2):
            swap(i, which).wait_send()
        hop(i).wait_send()
        forward(i).wait_send()


def hand_over(*refs):
    for i in range(3):
        refs[i + 3][...] = refs[i][...]


def on_device(q, k, v, o, g, lse, counts, wq, wk, wv):
    dma = pltpu.SemaphoreType.DMA
    hbm = pl.BlockSpec(memory_space=pl.ANY)
    blocks, units = NX * NZ, CAP // UNIT
    model = wq.shape[0]
    features = wq.shape[1] + wk.shape[1] + wv.shape[1]
    tile = (CAP, HD)
    flat = (units * HD, GROUP * UNIT)
    quarter = (CAP, model // 4)

    def vmem(shape, dtype=BF16):
        return pltpu.VMEM(shape, dtype)

    outs = pl.pallas_call(
        fused_kernel,
        name="attention_backward",
        out_shape=(
            jax.ShapeDtypeStruct(quarter, BF16),
            jax.ShapeDtypeStruct(tile, F32),
            jax.ShapeDtypeStruct(tile, F32),
        ),
        in_specs=[SMEM] + [VMEM] * 6 + [hbm] * 3,
        out_specs=(VMEM,) * 3,
        scratch_shapes=[
            vmem((blocks, 2) + tile),
            vmem((NY, CAP, GROUP * HD)),
            vmem((NY, CAP, GROUP * HD)),
            vmem((NY, 8, GROUP * UNIT), F32),
            vmem((blocks, HD, CAP)),
            vmem((blocks, 2) + tile, F32),
            vmem((NY, units, HD, GROUP * UNIT), F32),
            vmem((2, 2, CAP, GROUP * UNIT)), vmem((2, 2, CAP, GROUP * UNIT)),
            vmem((2, 2, 4) + tile), vmem((2, 2, 4) + tile),
            vmem((2, 2, 3) + tile), vmem((2, 2, 3) + tile),
            vmem((3, 2) + tile), vmem((3, 2) + tile),
            vmem(flat), vmem(flat), vmem((2,) + flat), vmem((2,) + flat),
            vmem((CAP, features)),
            vmem((CAP, model // 2)), vmem((CAP, model // 2)),
            vmem(quarter), vmem(quarter), vmem(quarter), vmem(quarter), vmem(quarter),
            vmem((model // TILE, TILE, features)),
            dma((2, 2, 2, 2, 4)), dma((2, 3, 2)), dma((2, 2, 2, 3)),
            dma((2, 2, 2, 2, 4)), dma((2, 3, 2)), dma((2, 2, 2)),
            dma((4, 2, PIECES)), dma((model // TILE, 3)),
        ],
        compiler_params=pltpu.CompilerParams(collective_id=0, has_side_effects=True),
    )(counts, k, v, q, g, o, lse, wq, wk, wv)
    return pl.pallas_call(
        hand_over,
        name="hand_over",
        out_shape=tuple(jax.ShapeDtypeStruct(a.shape, a.dtype) for a in outs),
        in_specs=[VMEM] * 3,
        out_specs=(VMEM,) * 3,
    )(*outs)


def solution(mesh):
    return jax.shard_map(
        on_device,
        mesh=mesh,
        in_specs=(
            P("ctx", "heads"), P("ctx", "heads"), P("ctx", "heads"), P("ctx", "heads"), P("ctx", "heads"),
            P("heads", "ctx"), P(), P(None, "heads"), P(None, "heads"), P(None, "heads"),
        ),
        out_specs=(P("ctx", "heads"), P("ctx", "heads"), P("ctx", "heads")),
        check_vma=False,
    )
```
